32 devices in a mesh: groups: 2 (over y), gx: 4 (over z), gy: 2 (over x), gz: 2 (over core).
Axes of the slice: x: 2, y: 2, z: 4, core: 2. Of those that a mesh axis runs over, the one named last changes fastest.
Arguments:
- pair: float32 [256, 48, 48], P(('groups', 'gz'), 'gx', 'gy'), parts along dimension 0, may hold values from -6 to 6
- residue_mask: int32 [96], P('groups'), parts along dimension 0, may hold values 0 or 1
- norm_in_gain: float32 [2, 128], P(None, 'gz'), may hold values from 0.25 to 1.75
- proj_weight: bfloat16 [2, 4, 128, 128], P(None, None, None, 'gz'), may hold values from -0.5 to 0.5
- gate_weight: bfloat16 [2, 128, 128], P(None, None, 'gz'), may hold values from -0.5 to 0.5
- norm_out_gain: float32 [2, 128], P(None, 'gz'), may hold values from 0.25 to 1.75
- out_weight: bfloat16 [2, 128, 128], P(None, None, 'gz'), may hold values from -0.5 to 0.5
Outputs:
- pair_out: float32 [256, 48, 48], P(('groups', 'gz'), 'gx', 'gy'), parts along dimension 0
The draws below stay inside these ranges and needn't reach their ends.
There are 2 independent parts, one for each index of `groups`. The reference program is written for one: setup_inputs(seed, part) draws one part's arguments, and reference() takes and returns one part's arrays. A program takes and returns all parts, laid end to end along the dimension named above; an argument that names none is the same for every part. Nothing has to cross between parts.
All inputs are finite; a program needn't handle non-finite values.
Results may differ from the reference program's by a relative error of at most 0.006.
Values may be sent and summed in bfloat16 or wider, within the bound.
No kernel may reach another device: no remote copies, remote signals or barrier semaphores. Data moves between devices by JAX's collectives and lax.ppermute only.
A program may use at most 64 MiB of HBM per device.

```python
import jax
import jax.numpy as jnp
from jax import lax

CHANNELS = 128
HIDDEN_SIZE = 128
RES = 48


def with_ends(entries, stream_key, smallest, top_value):
    extent = entries.shape
    index_at = [jax.random.randint(jax.random.fold_in(stream_key, axis), (), 0, extent[axis]) for axis in range(len(extent))]
    entries = entries.at[tuple(index_at)].set(smallest)
    longest = extent.index(max(extent))
    index_at[longest] = (index_at[longest] + 1) % extent[longest]
    return entries.at[tuple(index_at)].set(top_value)


def block_levels(rng, dims, split, least, largest):
    loudness = 1.0
    for dim, shards_of in split:
        heights = jax.random.uniform(jax.random.fold_in(jax.random.fold_in(rng, 6), dim), (shards_of,), jnp.float32, least / len(split), largest / len(split))
        loudness = loudness * jnp.repeat(jnp.exp(heights), dims[dim] // shards_of).reshape((-1,) + (1,) * (len(dims) - 1 - dim))
    return loudness


def gaussian(stream_key, shape, deviation, bound, cuts=(), dtype=jnp.bfloat16):
    result = jax.random.normal(stream_key, shape, jnp.float32) * deviation
    if len(cuts) > 0:
        result = block_levels(stream_key, shape, cuts, -0.22, 0.18) * result
    return jnp.clip(result, min=-bound, max=bound).astype(dtype)


def setup_inputs(seed: int = 0, part: int = 0) -> dict:
    key_of = jax.random.split(jax.random.key(seed), 8)
    own_keys = jax.random.split(jax.random.fold_in(key_of[7], part), 8)
    return {
        "pair": gaussian(own_keys[0], (CHANNELS, RES, RES), 1.0, 6.0, ((0, 2), (1, 4), (2, 2)), jnp.float32),
        "residue_mask": with_ends((jax.random.randint(own_keys[1], (RES,), 0, 4) < 3).astype(jnp.int32), jax.random.fold_in(own_keys[1], 1), 0, 1),
        "norm_in_gain": jnp.clip(1.0 + 0.15 * jax.random.normal(key_of[2], (2, CHANNELS), jnp.float32), 0.25, 1.75),
        "proj_weight": gaussian(key_of[3], (2, 4, CHANNELS, HIDDEN_SIZE), CHANNELS ** -0.5, 0.5, ((3, 2),)),
        "gate_weight": gaussian(key_of[4], (2, CHANNELS, CHANNELS), CHANNELS ** -0.5, 0.5, ((2, 2),)),
        "norm_out_gain": jnp.clip(1.0 + 0.15 * jax.random.normal(key_of[5], (2, HIDDEN_SIZE), jnp.float32), 0.25, 1.75),
        "out_weight": gaussian(key_of[6], (2, HIDDEN_SIZE, CHANNELS), HIDDEN_SIZE ** -0.5, 0.5, ((2, 2),)),
    }


EPSILON = 1e-05

def layer_norm(values, gain_row):
    mean_val = lax.optimization_barrier(jnp.mean(values, axis=0))
    centred = values - mean_val
    spread = lax.optimization_barrier(jnp.mean(centred * centred, axis=0))
    normed = (centred * lax.rsqrt(spread + EPSILON) * gain_row[:, None, None]).astype(jnp.bfloat16)
    return lax.optimization_barrier(normed).astype(jnp.float32)

def reference(pair, residue_mask, norm_in_gain, proj_weight, gate_weight, norm_out_gain, out_weight):
    residue_flags = residue_mask.astype(jnp.float32)
    pair_mask = residue_flags[:, None] * residue_flags[None, :]
    current = pair
    for update in range(2):
        normed = layer_norm(current, norm_in_gain[update])

        def project(which_one):
            return jnp.einsum('cij,ch->hij', normed, proj_weight[update, which_one].astype(jnp.float32))
        left = (jax.nn.sigmoid(project(0)) * project(1) * pair_mask).astype(jnp.bfloat16)
        left = lax.optimization_barrier(left).astype(jnp.float32)
        right = (jax.nn.sigmoid(project(2)) * project(3) * pair_mask).astype(jnp.bfloat16)
        right = lax.optimization_barrier(right).astype(jnp.float32)
        gate_values = jax.nn.sigmoid(jnp.einsum('cij,cd->dij', normed, gate_weight[update].astype(jnp.float32)))
        if update == 0:
            triangle = jnp.einsum('hik,hjk->hij', left, right)
        else:
            triangle = jnp.einsum('hki,hkj->hij', left, right)
        tri_normed = layer_norm(triangle, norm_out_gain[update])
        current = current + gate_values * jnp.einsum('hij,hd->dij', tri_normed, out_weight[update].astype(jnp.float32))
    return current
```

```python
import functools

import jax
import jax.numpy as jnp
from jax import lax
from jax.experimental import pallas as pl
from jax.experimental.pallas import tpu as pltpu
from jax.sharding import PartitionSpec as P

EPSILON = 1e-05
F32 = jnp.float32
BF16 = jnp.bfloat16
REPLICATED_LIMIT = 4 * 1024 * 1024


def sigmoid(x):
    return 0.5 * jnp.tanh(0.5 * x) + 0.5


def lane_norm(x, gain):
    mean = jnp.mean(x, axis=-1, keepdims=True)
    d = x - mean
    var = jnp.mean(d * d, axis=-1, keepdims=True)
    return d * lax.rsqrt(var + EPSILON) * gain


def dot(x, w):
    return jnp.dot(x.astype(BF16), w, preferred_element_type=F32)


def centre_kernel(own, other, out, *, half):
    core = lax.axis_index("gz")
    part, rows, cols = own.shape
    total = jnp.sum(own[...], axis=0) + jnp.sum(other[...], axis=0)
    mean = total * (1.0 / (2 * part))

    def emit(first, second, base):
        pieces = []
        for q in range(half):
            i = base + q
            both = jnp.concatenate([first[:, i, :], second[:, i, :]], axis=0)
            pieces.append(jnp.transpose(both - mean[i : i + 1, :]))
        out[...] = jnp.concatenate(pieces, axis=0).astype(BF16)

    @pl.when(core == 0)
    def _():
        emit(own, other, 0)

    @pl.when(core == 1)
    def _():
        emit(other, own, half)


def main_kernel(
    own, other, mask, gain_in, gain_out, wleft, wright, wgate, wout, pair, out,
    raw, normed, left, rightt, tri, first_update, znext, right1, left1, total,
    *, res, tile_rows, tile_cols, grid_rows, grid_cols,
):
    ch = mask.shape[1]
    half = tile_rows // 2
    ipad = -(-tile_rows // 8) * 8
    span = tile_cols + ipad
    row_block = lax.axis_index("gx")
    col_block = lax.axis_index("gy")
    core = lax.axis_index("gz")
    mk = mask[:res, :]

    for source, which in ((own, core), (other, 1 - core)):

        def norm_block(block, carry, source=source, which=which):
            x = source[block].astype(F32)
            var = jnp.mean(x * x, axis=-1, keepdims=True)
            zn = x * lax.rsqrt(var + EPSILON) * gain_in[0:1, :]
            base = (block // grid_cols * tile_rows + which * half) * res + block % grid_cols * tile_cols
            for q in range(half):
                at = pl.ds(pl.multiple_of(base + q * res, 8), tile_cols)
                raw[at, :] = x[q * tile_cols : (q + 1) * tile_cols]
                normed[at, :] = zn[q * tile_cols : (q + 1) * tile_cols]
            return carry

        lax.fori_loop(0, grid_rows * grid_cols, norm_block, 0)
    raw[pl.ds(res * res, 8), :] = jnp.zeros((8, ch), F32)
    normed[pl.ds(res * res, 8), :] = jnp.zeros((8, ch), F32)

    def gated(x, w):
        p = dot(x, w)
        return sigmoid(p[:, :ch]) * p[:, ch:]

    step = 8

    def left_block(block, carry):
        at = pl.ds(pl.multiple_of(block * step * res, 8), step * res)
        y = gated(normed[at, :], wleft[0]).reshape(step, res, ch)
        rows = mask[pl.ds(pl.multiple_of(block * step, 8), step), :]
        y = y * mk[None] * rows[:, None, :]
        left[at, :] = y.reshape(step * res, ch)
        return carry

    lax.fori_loop(0, res // step, left_block, 0)

    rightt[...] = jnp.zeros_like(rightt)
    group = 4

    def right_rows(first, slot, count):
        def block(n, carry):
            x = normed[pl.ds(pl.multiple_of((first + n * group) * res, 8), group * res), :]
            y = gated(x, wright[0])
            for q in range(group):
                row = mask[pl.ds(first + n * group + q, 1), :]
                v = y[q * res : (q + 1) * res] * mk * row
                rightt[pl.ds(slot + n * group + q, res, stride=span), :] = v
            return carry

        lax.fori_loop(0, count // group, block, 0)

    right_rows(col_block * tile_cols, 0, tile_cols)
    right_rows(row_block * tile_rows, tile_cols, tile_rows)

    block_rows = 4

    def tri_block(n, carry):
        accs = [jnp.zeros((span, ch), F32) for _ in range(block_rows)]
        for k in range(res):
            r = rightt[k * span : (k + 1) * span, :]
            for q in range(block_rows):
                accs[q] = accs[q] + left[pl.ds((n * block_rows + q) * res + k, 1), :] * r
        for q in range(block_rows):
            at = pl.ds(pl.multiple_of((n * block_rows + q) * span, 8), span)
            tri[at, :] = lane_norm(accs[q], gain_out[0:1, :])
        return carry

    lax.fori_loop(0, res // block_rows, tri_block, 0)

    wide = 8

    def out_block(n, carry):
        zs, ns = [], []
        for q in range(wide):
            r = n * wide + q
            at_cols = pl.ds(pl.multiple_of(r * res + col_block * tile_cols, 8), tile_cols)
            at_rows = pl.ds(r * res + row_block * tile_rows, ipad)
            zs += [raw[at_cols, :], raw[at_rows, :]]
            ns += [normed[at_cols, :], normed[at_rows, :]]
        at = pl.ds(pl.multiple_of(n * wide * span, 8), wide * span)
        gate = sigmoid(dot(jnp.concatenate(ns, axis=0), wgate[0]))
        update = gate * dot(tri[at, :], wout[0])
        first_update[at, :] = update
        znext[at, :] = lane_norm(jnp.concatenate(zs, axis=0) + update, gain_in[1:2, :])
        return carry

    lax.fori_loop(0, res // wide, out_block, 0)

    def second_block(n, carry):
        rs, ls = [], []
        for q in range(wide):
            at = (n * wide + q) * span
            rs.append(znext[pl.ds(pl.multiple_of(at, 8), tile_cols), :])
            ls.append(znext[pl.ds(pl.multiple_of(at + tile_cols, 8), ipad), :])
        rows = mask[pl.ds(pl.multiple_of(n * wide, 8), wide), :][:, None, :]
        cmask = mask[pl.ds(pl.multiple_of(col_block * tile_cols, 8), tile_cols), :]
        imask = mask[pl.ds(row_block * tile_rows, ipad), :]
        r = gated(jnp.concatenate(rs, axis=0), wright[1]).reshape(wide, tile_cols, ch)
        r = r * rows * cmask[None]
        right1[pl.ds(pl.multiple_of(n * wide * tile_cols, 8), wide * tile_cols), :] = r.reshape(wide * tile_cols, ch)
        v = gated(jnp.concatenate(ls, axis=0), wleft[1]).reshape(wide, ipad, ch)
        v = v * rows * imask[None]
        left1[pl.ds(pl.multiple_of(n * wide * ipad, 8), wide * ipad), :] = v.reshape(wide * ipad, ch)
        return carry

    lax.fori_loop(0, res // wide, second_block, 0)

    def tri1_block(k, accs):
        r = right1[pl.ds(pl.multiple_of(k * tile_cols, 8), tile_cols), :]
        return tuple(
            acc + left1[pl.ds(k * ipad + i, 1), :] * r for i, acc in enumerate(accs)
        )

    accs = lax.fori_loop(
        0, res, tri1_block, tuple(jnp.zeros((tile_cols, ch), F32) for _ in range(tile_rows)), unroll=4
    )
    tn = jnp.concatenate([lane_norm(acc, gain_out[1:2, :]) for acc in accs], axis=0)
    ns, us = [], []
    for i in range(tile_rows):
        at = pl.ds(pl.multiple_of((row_block * tile_rows + i) * span, 8), tile_cols)
        ns.append(znext[at, :])
        us.append(first_update[at, :])
    gate = sigmoid(dot(jnp.concatenate(ns, axis=0), wgate[1]))
    total[...] = jnp.concatenate(us, axis=0) + gate * dot(tn, wout[1])
    part = ch // 2
    for i in range(tile_rows):
        t = pltpu.roll(total[i * tile_cols : (i + 1) * tile_cols, :], core * part, 1)
        out[:, i, :] = pair[:, i, :] + jnp.transpose(t)[:part]


def swap_cores(x):
    return lax.ppermute(x, "gz", [(0, 1), (1, 0)])


def join_cores(own, other, axis):
    first = jnp.concatenate([own, other], axis=axis)
    second = jnp.concatenate([other, own], axis=axis)
    return jnp.where(lax.axis_index("gz") == 0, first, second)


def replicated(
    pair, residue_mask, norm_in_gain, proj_weight, gate_weight, norm_out_gain, out_weight
):
    part, tile_rows, tile_cols = pair.shape
    grid_rows, grid_cols = lax.axis_size("gx"), lax.axis_size("gy")
    res = residue_mask.shape[0]
    ch = 2 * part
    half = tile_rows // 2
    ipad = -(-tile_rows // 8) * 8
    span = tile_cols + ipad

    own_weights = jnp.concatenate(
        [proj_weight, gate_weight[:, None], out_weight[:, None]], axis=1
    )
    own_gains = jnp.concatenate([norm_in_gain, norm_out_gain], axis=0)
    other_pair = swap_cores(pair)
    weights = join_cores(own_weights, swap_cores(own_weights), 3)
    gains = join_cores(own_gains, swap_cores(own_gains), 1)

    message = pl.pallas_call(
        functools.partial(centre_kernel, half=half),
        out_shape=jax.ShapeDtypeStruct((half * tile_cols, ch), BF16),
        name="centre",
    )(pair, other_pair)
    chips = grid_rows * grid_cols
    gathered = lax.all_to_all(
        jnp.broadcast_to(message[None], (chips,) + message.shape), ("gx", "gy"), 0, 0
    )
    other_gathered = swap_cores(gathered)

    wleft = jnp.concatenate([weights[:, 0], weights[:, 1]], axis=2)
    wright = jnp.concatenate([weights[:, 2], weights[:, 3]], axis=2)
    mask = jnp.pad(residue_mask.astype(F32), (0, 8))
    mask = jnp.broadcast_to(mask[:, None], (res + 8, ch))
    vmem = lambda rows: pltpu.VMEM((rows, ch), F32)
    return pl.pallas_call(
        functools.partial(
            main_kernel,
            res=res,
            tile_rows=tile_rows,
            tile_cols=tile_cols,
            grid_rows=grid_rows,
            grid_cols=grid_cols,
        ),
        out_shape=jax.ShapeDtypeStruct(pair.shape, F32),
        scratch_shapes=[
            vmem(res * res + 8),
            vmem(res * res + 8),
            vmem(res * res),
            vmem(res * span),
            vmem(res * span),
            vmem(res * span),
            vmem(res * span),
            vmem(res * tile_cols),
            vmem(res * ipad),
            vmem(tile_rows * tile_cols),
        ],
        compiler_params=pltpu.CompilerParams(vmem_limit_bytes=48 * 1024 * 1024),
        name="update",
    )(
        gathered, other_gathered, mask, gains[:2], gains[2:], wleft, wright,
        weights[:, 4], weights[:, 5], pair,
    )


def layer_norm_gathered(values, gain_part):
    full_values, full_gain = (
        lax.all_gather(values, "gz", axis=0, tiled=True),
        lax.all_gather(gain_part, "gz", axis=0, tiled=True),
    )
    mean_val = jnp.mean(full_values, axis=0)
    centred = full_values - mean_val
    spread = jnp.mean(centred * centred, axis=0)
    result = (centred * lax.rsqrt(spread + EPSILON) * full_gain[:, None, None]).astype(jnp.bfloat16)
    return result


def transpose_tile(pair_tile):
    depth_dim, tile_rows, tile_cols = pair_tile.shape
    across = lax.axis_size("gy")
    down_size = lax.axis_size("gx")
    quarter = tile_rows // across
    spread_rows = lax.all_to_all(pair_tile, "gy", split_axis=1, concat_axis=2, tiled=True)
    blocks = spread_rows.reshape(depth_dim, quarter, down_size, tile_rows)
    blocks = jnp.transpose(blocks, (0, 3, 2, 1))[:, :, :, None, :]
    moved_back = lax.all_to_all(
        lax.all_to_all(blocks, "gx", split_axis=2, concat_axis=2, tiled=True),
        "gy",
        split_axis=2,
        concat_axis=3,
        tiled=True,
    )
    return moved_back.reshape(depth_dim, tile_rows, tile_cols)


def fold_panels(left_tile, right_tile):
    left_panel = lax.all_gather(left_tile, "gy", axis=2, tiled=True)
    return jnp.einsum(
        "hik,hkj->hij",
        left_panel,
        lax.all_gather(right_tile, "gx", axis=1, tiled=True),
        preferred_element_type=jnp.float32,
    )


def distributed(
    pair, residue_mask, norm_in_gain, proj_weight, gate_weight, norm_out_gain, out_weight
):
    tile_rows = pair.shape[1]
    tile_cols = pair.shape[2]
    row_start = lax.axis_index("gx") * tile_rows
    col_start = lax.axis_index("gy") * tile_cols
    row_flags = lax.dynamic_slice_in_dim(residue_mask, row_start, tile_rows).astype(jnp.float32)
    col_flags = lax.dynamic_slice_in_dim(residue_mask, col_start, tile_cols).astype(jnp.float32)
    pair_mask = row_flags[:, None] * col_flags[None, :]
    current = pair
    for update in range(2):
        normed = layer_norm_gathered(current, norm_in_gain[update])
        projected = jnp.einsum(
            "cij,pch->phij", normed, proj_weight[update], preferred_element_type=jnp.float32
        )
        left_tile = (jax.nn.sigmoid(projected[0]) * projected[1] * pair_mask).astype(jnp.bfloat16)
        right_tile = (jax.nn.sigmoid(projected[2]) * projected[3] * pair_mask).astype(jnp.bfloat16)
        gate_values = jax.nn.sigmoid(
            jnp.einsum(
                "cij,cd->dij", normed, gate_weight[update], preferred_element_type=jnp.float32
            )
        )
        if update == 0:
            triangle = fold_panels(left_tile, transpose_tile(right_tile))
        else:
            triangle = fold_panels(transpose_tile(left_tile), right_tile)
        tri_normed = layer_norm_gathered(triangle, norm_out_gain[update])
        current = current + gate_values * jnp.einsum(
            "hij,hd->dij", tri_normed, out_weight[update], preferred_element_type=jnp.float32
        )
    return current


def fits_replicated(pair, residue_mask):
    part, tile_rows, tile_cols = pair.shape
    res = residue_mask.shape[0]
    return (
        lax.axis_size("gz") == 2
        and res * res * part * 2 * 4 <= REPLICATED_LIMIT
        and res % 8 == 0
        and tile_rows % 4 == 0
        and tile_cols % 8 == 0
    )


def per_device(pair, residue_mask, *parameters):
    plan = replicated if fits_replicated(pair, residue_mask) else distributed
    return plan(pair, residue_mask, *parameters)


def solution(mesh):
    return jax.shard_map(
        per_device,
        mesh=mesh,
        in_specs=(
            P(("groups", "gz"), "gx", "gy"),
            P("groups"),
            P(None, "gz"),
            P(None, None, None, "gz"),
            P(None, None, "gz"),
            P(None, "gz"),
            P(None, None, "gz"),
        ),
        out_specs=P(("groups", "gz"), "gx", "gy"),
        check_vma=False,
    )
```

```python
import functools

import jax
import jax.numpy as jnp
from jax import lax
from jax.experimental import pallas as pl
from jax.experimental.pallas import tpu as pltpu
from jax.sharding import PartitionSpec as P

EPSILON = 1e-05
F32 = jnp.float32
BF16 = jnp.bfloat16
REPLICATED_LIMIT = 4 * 1024 * 1024


def sigmoid(x):
    return 0.5 * jnp.tanh(0.5 * x) + 0.5


def lane_norm(x, gain):
    mean = jnp.mean(x, axis=-1, keepdims=True)
    d = x - mean
    var = jnp.mean(d * d, axis=-1, keepdims=True)
    return d * lax.rsqrt(var + EPSILON) * gain


def dot(x, w):
    return jnp.dot(x.astype(BF16), w, preferred_element_type=F32)


def centre_kernel(own, other, out, *, half):
    core = lax.axis_index("gz")
    part = own.shape[2]
    pairs = half * own.shape[1]
    rows = pl.ds(core * half, half)
    both = jnp.concatenate(
        [own[rows].reshape(pairs, part), other[rows].reshape(pairs, part)], axis=1
    )
    both = pltpu.roll(both, core * part, 1)
    message = (both - jnp.mean(both, axis=-1, keepdims=True)).astype(BF16)
    for chip in range(out.shape[0]):
        out[chip] = message


def main_kernel(
    own, other, mask, gain_in, gain_out, wleft, wright, wgate, wout, pair, out,
    raw, normed, left, rightt, tri, first_update, znext, right1, left1,
    *, res, tile_rows, tile_cols, grid_rows, grid_cols,
):
    ch = mask.shape[1]
    half = tile_rows // 2
    ipad = -(-tile_rows // 8) * 8
    span = tile_cols + ipad
    row_block = lax.axis_index("gx")
    col_block = lax.axis_index("gy")
    core = lax.axis_index("gz")
    mk = mask[:res, :]

    for source, which in ((own, core), (other, 1 - core)):

        def norm_block(block, carry, source=source, which=which):
            x = source[block].astype(F32)
            var = jnp.mean(x * x, axis=-1, keepdims=True)
            zn = x * lax.rsqrt(var + EPSILON) * gain_in[0:1, :]
            base = (block // grid_cols * tile_rows + which * half) * res + block % grid_cols * tile_cols
            for q in range(half):
                at = pl.ds(pl.multiple_of(base + q * res, 8), tile_cols)
                raw[at, :] = x[q * tile_cols : (q + 1) * tile_cols]
                normed[at, :] = zn[q * tile_cols : (q + 1) * tile_cols]
            return carry

        lax.fori_loop(0, grid_rows * grid_cols, norm_block, 0)
    raw[pl.ds(res * res, 8), :] = jnp.zeros((8, ch), F32)
    normed[pl.ds(res * res, 8), :] = jnp.zeros((8, ch), F32)

    def gated(x, w):
        p = dot(x, w)
        return sigmoid(p[:, :ch]) * p[:, ch:]

    step = 8

    def left_block(block, carry):
        at = pl.ds(pl.multiple_of(block * step * res, 8), step * res)
        y = gated(normed[at, :], wleft[0]).reshape(step, res, ch)
        rows = mask[pl.ds(pl.multiple_of(block * step, 8), step), :]
        y = y * mk[None] * rows[:, None, :]
        left[at, :] = y.reshape(step * res, ch)
        return carry

    lax.fori_loop(0, res // step, left_block, 0)

    rightt[...] = jnp.zeros_like(rightt)
    group = 4

    def right_rows(first, slot, count):
        def block(n, carry):
            x = normed[pl.ds(pl.multiple_of((first + n * group) * res, 8), group * res), :]
            y = gated(x, wright[0])
            for q in range(group):
                row = mask[pl.ds(first + n * group + q, 1), :]
                v = y[q * res : (q + 1) * res] * mk * row
                rightt[pl.ds(slot + n * group + q, res, stride=span), :] = v
            return carry

        lax.fori_loop(0, count // group, block, 0)

    right_rows(col_block * tile_cols, 0, tile_cols)
    right_rows(row_block * tile_rows, tile_cols, tile_rows)

    block_rows = 4

    def tri_block(n, carry):
        accs = [jnp.zeros((span, ch), F32) for _ in range(block_rows)]
        for k in range(res):
            r = rightt[k * span : (k + 1) * span, :]
            for q in range(block_rows):
                accs[q] = accs[q] + left[pl.ds((n * block_rows + q) * res + k, 1), :] * r
        for q in range(block_rows):
            at = pl.ds(pl.multiple_of((n * block_rows + q) * span, 8), span)
            tri[at, :] = lane_norm(accs[q], gain_out[0:1, :])
        return carry

    lax.fori_loop(0, res // block_rows, tri_block, 0)

    wide = 8

    def out_block(n, carry):
        zs, ns = [], []
        for q in range(wide):
            r = n * wide + q
            at_cols = pl.ds(pl.multiple_of(r * res + col_block * tile_cols, 8), tile_cols)
            at_rows = pl.ds(r * res + row_block * tile_rows, ipad)
            zs += [raw[at_cols, :], raw[at_rows, :]]
            ns += [normed[at_cols, :], normed[at_rows, :]]
        at = pl.ds(pl.multiple_of(n * wide * span, 8), wide * span)
        gate = sigmoid(dot(jnp.concatenate(ns, axis=0), wgate[0]))
        update = gate * dot(tri[at, :], wout[0])
        first_update[at, :] = update
        znext[at, :] = lane_norm(jnp.concatenate(zs, axis=0) + update, gain_in[1:2, :])
        return carry

    lax.fori_loop(0, res // wide, out_block, 0)

    def second_block(n, carry):
        rs, ls = [], []
        for q in range(wide):
            at = (n * wide + q) * span
            rs.append(znext[pl.ds(pl.multiple_of(at, 8), tile_cols), :])
            ls.append(znext[pl.ds(pl.multiple_of(at + tile_cols, 8), ipad), :])
        rows = mask[pl.ds(pl.multiple_of(n * wide, 8), wide), :][:, None, :]
        cmask = mask[pl.ds(pl.multiple_of(col_block * tile_cols, 8), tile_cols), :]
        imask = mask[pl.ds(row_block * tile_rows, ipad), :]
        r = gated(jnp.concatenate(rs, axis=0), wright[1]).reshape(wide, tile_cols, ch)
        r = r * rows * cmask[None]
        right1[pl.ds(pl.multiple_of(n * wide * tile_cols, 8), wide * tile_cols), :] = r.reshape(wide * tile_cols, ch)
        v = gated(jnp.concatenate(ls, axis=0), wleft[1]).reshape(wide, ipad, ch)
        v = v * rows * imask[None]
        left1[pl.ds(pl.multiple_of(n * wide * ipad, 8), wide * ipad), :] = v.reshape(wide * ipad, ch)
        return carry

    lax.fori_loop(0, res // wide, second_block, 0)

    def tri1_block(k, accs):
        r = right1[pl.ds(pl.multiple_of(k * tile_cols, 8), tile_cols), :]
        return tuple(
            acc + left1[pl.ds(k * ipad + i, 1), :] * r for i, acc in enumerate(accs)
        )

    accs = lax.fori_loop(
        0, res, tri1_block, tuple(jnp.zeros((tile_cols, ch), F32) for _ in range(tile_rows)), unroll=4
    )
    tn = jnp.concatenate([lane_norm(acc, gain_out[1:2, :]) for acc in accs], axis=0)
    ns, us = [], []
    for i in range(tile_rows):
        at = pl.ds(pl.multiple_of((row_block * tile_rows + i) * span, 8), tile_cols)
        ns.append(znext[at, :])
        us.append(first_update[at, :])
    gate = sigmoid(dot(jnp.concatenate(ns, axis=0), wgate[1]))
    moved = jnp.concatenate(us, axis=0) + gate * dot(tn, wout[1])
    part = ch // 2
    moved = pltpu.roll(moved, core * part, 1)[:, :part]
    out[...] = pair[...] + moved.reshape(tile_rows, tile_cols, part)


def swap_cores(x):
    return lax.ppermute(x, "gz", [(0, 1), (1, 0)])


def join_cores(own, other, axis):
    first = jnp.concatenate([own, other], axis=axis)
    second = jnp.concatenate([other, own], axis=axis)
    return jnp.where(lax.axis_index("gz") == 0, first, second)


def replicated(
    pair, residue_mask, norm_in_gain, proj_weight, gate_weight, norm_out_gain, out_weight
):
    part, tile_rows, tile_cols = pair.shape
    tile = jnp.transpose(pair, (1, 2, 0))
    grid_rows, grid_cols = lax.axis_size("gx"), lax.axis_size("gy")
    res = residue_mask.shape[0]
    ch = 2 * part
    half = tile_rows // 2
    ipad = -(-tile_rows // 8) * 8
    span = tile_cols + ipad

    own_weights = jnp.concatenate(
        [proj_weight, gate_weight[:, None], out_weight[:, None]], axis=1
    )
    own_gains = jnp.concatenate([norm_in_gain, norm_out_gain], axis=0)
    other_tile = swap_cores(tile)
    weights = join_cores(own_weights, swap_cores(own_weights), 3)
    gains = join_cores(own_gains, swap_cores(own_gains), 1)

    chips = grid_rows * grid_cols
    message = pl.pallas_call(
        functools.partial(centre_kernel, half=half),
        out_shape=jax.ShapeDtypeStruct((chips, half * tile_cols, ch), BF16),
        compiler_params=pltpu.CompilerParams(vmem_limit_bytes=4 * 1024 * 1024),
        name="centre",
    )(tile, other_tile)
    gathered = lax.all_to_all(message, ("gx", "gy"), 0, 0)
    other_gathered = swap_cores(gathered)

    wleft = jnp.concatenate([weights[:, 0], weights[:, 1]], axis=2)
    wright = jnp.concatenate([weights[:, 2], weights[:, 3]], axis=2)
    mask = jnp.pad(residue_mask.astype(F32), (0, 8))
    mask = jnp.broadcast_to(mask[:, None], (res + 8, ch))
    vmem = lambda rows: pltpu.VMEM((rows, ch), F32)
    result = pl.pallas_call(
        functools.partial(
            main_kernel,
            res=res,
            tile_rows=tile_rows,
            tile_cols=tile_cols,
            grid_rows=grid_rows,
            grid_cols=grid_cols,
        ),
        out_shape=jax.ShapeDtypeStruct(tile.shape, F32),
        scratch_shapes=[
            vmem(res * res + 8),
            vmem(res * res + 8),
            vmem(res * res),
            vmem(res * span),
            vmem(res * span),
            vmem(res * span),
            vmem(res * span),
            vmem(res * tile_cols),
            vmem(res * ipad),
        ],
        compiler_params=pltpu.CompilerParams(vmem_limit_bytes=24 * 1024 * 1024),
        name="update",
    )(
        gathered, other_gathered, mask, gains[:2], gains[2:], wleft, wright,
        weights[:, 4], weights[:, 5], tile,
    )
    return jnp.transpose(result, (2, 0, 1))


def layer_norm_gathered(values, gain_part):
    full_values, full_gain = (
        lax.all_gather(values, "gz", axis=0, tiled=True),
        lax.all_gather(gain_part, "gz", axis=0, tiled=True),
    )
    mean_val = jnp.mean(full_values, axis=0)
    centred = full_values - mean_val
    spread = jnp.mean(centred * centred, axis=0)
    result = (centred * lax.rsqrt(spread + EPSILON) * full_gain[:, None, None]).astype(jnp.bfloat16)
    return result


def transpose_tile(pair_tile):
    depth_dim, tile_rows, tile_cols = pair_tile.shape
    across = lax.axis_size("gy")
    down_size = lax.axis_size("gx")
    quarter = tile_rows // across
    spread_rows = lax.all_to_all(pair_tile, "gy", split_axis=1, concat_axis=2, tiled=True)
    blocks = spread_rows.reshape(depth_dim, quarter, down_size, tile_rows)
    blocks = jnp.transpose(blocks, (0, 3, 2, 1))[:, :, :, None, :]
    moved_back = lax.all_to_all(
        lax.all_to_all(blocks, "gx", split_axis=2, concat_axis=2, tiled=True),
        "gy",
        split_axis=2,
        concat_axis=3,
        tiled=True,
    )
    return moved_back.reshape(depth_dim, tile_rows, tile_cols)


def fold_panels(left_tile, right_tile):
    left_panel = lax.all_gather(left_tile, "gy", axis=2, tiled=True)
    return jnp.einsum(
        "hik,hkj->hij",
        left_panel,
        lax.all_gather(right_tile, "gx", axis=1, tiled=True),
        preferred_element_type=jnp.float32,
    )


def distributed(
    pair, residue_mask, norm_in_gain, proj_weight, gate_weight, norm_out_gain, out_weight
):
    tile_rows = pair.shape[1]
    tile_cols = pair.shape[2]
    row_start = lax.axis_index("gx") * tile_rows
    col_start = lax.axis_index("gy") * tile_cols
    row_flags = lax.dynamic_slice_in_dim(residue_mask, row_start, tile_rows).astype(jnp.float32)
    col_flags = lax.dynamic_slice_in_dim(residue_mask, col_start, tile_cols).astype(jnp.float32)
    pair_mask = row_flags[:, None] * col_flags[None, :]
    current = pair
    for update in range(2):
        normed = layer_norm_gathered(current, norm_in_gain[update])
        projected = jnp.einsum(
            "cij,pch->phij", normed, proj_weight[update], preferred_element_type=jnp.float32
        )
        left_tile = (jax.nn.sigmoid(projected[0]) * projected[1] * pair_mask).astype(jnp.bfloat16)
        right_tile = (jax.nn.sigmoid(projected[2]) * projected[3] * pair_mask).astype(jnp.bfloat16)
        gate_values = jax.nn.sigmoid(
            jnp.einsum(
                "cij,cd->dij", normed, gate_weight[update], preferred_element_type=jnp.float32
            )
        )
        if update == 0:
            triangle = fold_panels(left_tile, transpose_tile(right_tile))
        else:
            triangle = fold_panels(transpose_tile(left_tile), right_tile)
        tri_normed = layer_norm_gathered(triangle, norm_out_gain[update])
        current = current + gate_values * jnp.einsum(
            "hij,hd->dij", tri_normed, out_weight[update], preferred_element_type=jnp.float32
        )
    return current


def fits_replicated(pair, residue_mask):
    part, tile_rows, tile_cols = pair.shape
    res = residue_mask.shape[0]
    return (
        lax.axis_size("gz") == 2
        and res * res * part * 2 * 4 <= REPLICATED_LIMIT
        and res % 8 == 0
        and tile_rows % 4 == 0
        and tile_cols % 8 == 0
    )


def per_device(pair, residue_mask, *parameters):
    plan = replicated if fits_replicated(pair, residue_mask) else distributed
    return plan(pair, residue_mask, *parameters)


def solution(mesh):
    return jax.shard_map(
        per_device,
        mesh=mesh,
        in_specs=(
            P(("groups", "gz"), "gx", "gy"),
            P("groups"),
            P(None, "gz"),
            P(None, None, None, "gz"),
            P(None, None, "gz"),
            P(None, "gz"),
            P(None, None, "gz"),
        ),
        out_specs=P(("groups", "gz"), "gx", "gy"),
        check_vma=False,
    )
```

```python
import functools

import jax
import jax.numpy as jnp
from jax import lax
from jax.experimental import pallas as pl
from jax.experimental.pallas import tpu as pltpu
from jax.sharding import PartitionSpec as P

EPSILON = 1e-05
F32 = jnp.float32
BF16 = jnp.bfloat16
REPLICATED_LIMIT = 4 * 1024 * 1024


def dot(x, w):
    return jnp.dot(x.astype(BF16), w, preferred_element_type=F32)


def lane_norm(x, gain, ones):
    d = x - jnp.mean(x, axis=-1, keepdims=True)
    return d * lax.rsqrt(dot(d * d, ones) + EPSILON) * gain


def gated(x, w):
    p = dot(x, w)
    ch = p.shape[1] // 2
    return (jnp.tanh(p[:, :ch]) + 1.0) * p[:, ch:]


def steps(total, size, body, unrolled=False):
    if unrolled or size >= total:
        for first in range(0, total, size):
            body(first)
    else:

        def step(n, carry):
            body(pl.multiple_of(n * size, size))
            return carry

        lax.fori_loop(0, total // size, step, 0)


def rows_at(first, count):
    return pl.ds(first if isinstance(first, int) else pl.multiple_of(first, 8), count)


def centre_kernel(own, other, out, *, half):
    core = lax.axis_index("gz")
    part = own.shape[2]
    pairs = half * own.shape[1]
    rows = pl.ds(core * half, half)
    both = jnp.concatenate(
        [own[rows].reshape(pairs, part), other[rows].reshape(pairs, part)], axis=1
    )
    both = pltpu.roll(both, core * part, 1)
    message = (both - jnp.mean(both, axis=-1, keepdims=True)).astype(BF16)
    for chip in range(out.shape[0]):
        out[chip] = message


def weights_kernel(own, other, own_gains, other_gains, flags, wleft, wright, wgate, wout, gains, mask):
    core = lax.axis_index("gz")
    half = own.shape[2]
    for u in range(2):
        for p in range(6):
            mine, theirs = own[u, p].astype(F32) * 0.5, other[u, p].astype(F32) * 0.5
            first = jnp.where(core == 0, mine, theirs)
            second = jnp.where(core == 0, theirs, mine)
            full = jnp.transpose(jnp.concatenate([first, second], axis=0)).astype(BF16)
            if p < 2:
                wleft[u, :, p * 2 * half : (p + 1) * 2 * half] = full
            elif p < 4:
                wright[u, :, (p - 2) * 2 * half : (p - 1) * 2 * half] = full
            elif p == 4:
                wgate[u] = full
            else:
                wout[u] = full
    gains[...] = pltpu.roll(jnp.concatenate([own_gains[...], other_gains[...]], axis=1), core * half, 1)
    row = flags[...].astype(F32)
    size = row.shape[1]
    wide = jnp.transpose(jnp.broadcast_to(row, (mask.shape[1], size)))
    mask[...] = jnp.zeros_like(mask)
    mask[:size, :] = wide


def main_kernel(
    own, other, mask, gains, wleft, wright, wgate, wout, pair, out,
    raw, normed, left, rightt, tri, first_update, znext, right1, left1,
    *, res, tile_rows, tile_cols, grid_rows, grid_cols, sizes,
):
    ch = mask.shape[1]
    half = tile_rows // 2
    ipad = -(-tile_rows // 8) * 8
    span = tile_cols + ipad
    row_block = lax.axis_index("gx")
    col_block = lax.axis_index("gy")
    core = lax.axis_index("gz")
    first_col = col_block * tile_cols
    first_row = row_block * tile_rows
    ones = jnp.full((ch, ch), 1.0 / ch, BF16)
    gain_in, gain_out = gains[0:2, :], gains[2:4, :]

    def norm_block(block):
        for n in range(sizes["norm"]):
            at_block = block + n
            for source, which in ((own, core), (other, 1 - core)):
                x = source[at_block].astype(F32)
                var = jnp.mean(x * x, axis=-1, keepdims=True)
                zn = x * lax.rsqrt(var + EPSILON) * gain_in[0:1]
                base = (at_block // grid_cols * tile_rows + which * half) * res
                base = base + at_block % grid_cols * tile_cols
                for q in range(half):
                    at = pl.ds(pl.multiple_of(base + q * res, 8), tile_cols)
                    raw[at, :] = x[q * tile_cols : (q + 1) * tile_cols]
                    normed[at, :] = zn[q * tile_cols : (q + 1) * tile_cols]

    steps(grid_rows * grid_cols, sizes["norm"], norm_block)
    raw[pl.ds(res * res, 8), :] = jnp.zeros((8, ch), F32)
    normed[pl.ds(res * res, 8), :] = jnp.zeros((8, ch), F32)

    def left_block(first):
        count = sizes["left"]
        at = rows_at(first * res, count * res)
        y = gated(normed[at, :], wleft[0]).reshape(count, res, ch) * mask[:res, :][None]
        left[at, :] = y.reshape(count * res, ch)

    steps(res, sizes["left"], left_block)

    for k in range(ipad - tile_rows):
        rightt[pl.ds(tile_cols + tile_rows + k, res, stride=span), :] = jnp.zeros((res, ch), F32)

    def right_block(slot):
        count = sizes["right"]
        row = first_col + slot if slot < tile_cols else first_row + slot - tile_cols
        y = gated(normed[rows_at(row * res, count * res), :], wright[0])
        for q in range(count):
            rightt[pl.ds(slot + q, res, stride=span), :] = y[q * res : (q + 1) * res]

    steps(tile_cols + tile_rows, sizes["right"], right_block, unrolled=True)

    def tri_block(first):
        count = sizes["tri"]

        def add(k, accs):
            r = rightt[pl.ds(pl.multiple_of(k * span, 8), span), :]
            return tuple(acc + left[pl.ds((first + q) * res + k, 1), :] * r for q, acc in enumerate(accs))

        accs = lax.fori_loop(
            0, res, add, tuple(jnp.zeros((span, ch), F32) for _ in range(count)), unroll=sizes["unroll"]
        )
        for q in range(count):
            tri[rows_at((first + q) * span, span), :] = accs[q]

    steps(res, sizes["tri"], tri_block)

    smask = jnp.concatenate(
        [mask[rows_at(first_col, tile_cols), :], mask[pl.ds(first_row, ipad), :]], axis=0
    )

    def out_block(first):
        count = sizes["out"]
        zs, ns, ms = [], [], []
        for q in range(count):
            r = first + q
            at_cols = pl.ds(pl.multiple_of(r * res + first_col, 8), tile_cols)
            at_rows = pl.ds(r * res + first_row, ipad)
            zs += [raw[at_cols, :], raw[at_rows, :]]
            ns += [normed[at_cols, :], normed[at_rows, :]]
            ms.append(smask * mask[pl.ds(r, 1), :])
        at = rows_at(first * span, count * span)
        gate = jnp.tanh(dot(jnp.concatenate(ns, axis=0), wgate[0])) + 1.0
        tn = lane_norm(tri[at, :], gain_out[0:1], ones)
        update = gate * dot(tn, wout[0]) * jnp.concatenate(ms, axis=0)
        first_update[at, :] = update
        znext[at, :] = lane_norm(jnp.concatenate(zs, axis=0) + update, gain_in[1:2], ones)

    steps(res, sizes["out"], out_block)

    def second_block(first):
        count = sizes["second"]
        rs, ls = [], []
        for q in range(count):
            at = (first + q) * span
            rs.append(znext[rows_at(at, tile_cols), :])
            ls.append(znext[rows_at(at + tile_cols, ipad), :])
        rows = mask[rows_at(first, count), :]
        at = rows_at(first * tile_cols, count * tile_cols)
        right1[at, :] = gated(jnp.concatenate(rs, axis=0), wright[1])
        v = gated(jnp.concatenate(ls, axis=0), wleft[1]).reshape(count, ipad, ch) * rows[:, None, :]
        left1[rows_at(first * ipad, count * ipad), :] = v.reshape(count * ipad, ch)

    steps(res, sizes["second"], second_block)

    def tri1_block(k, accs):
        r = right1[pl.ds(pl.multiple_of(k * tile_cols, 8), tile_cols), :]
        return tuple(acc + left1[pl.ds(k * ipad + i, 1), :] * r for i, acc in enumerate(accs))

    accs = lax.fori_loop(
        0, res, tri1_block, tuple(jnp.zeros((tile_cols, ch), F32) for _ in range(tile_rows)), unroll=4
    )
    tn = lane_norm(jnp.concatenate(accs, axis=0), gain_out[1:2], ones)
    ns, us, ms = [], [], []
    for i in range(tile_rows):
        at = pl.ds(pl.multiple_of((first_row + i) * span, 8), tile_cols)
        ns.append(znext[at, :])
        us.append(first_update[at, :])
        ms.append(smask[:tile_cols] * mask[pl.ds(first_row + i, 1), :])
    gate = jnp.tanh(dot(jnp.concatenate(ns, axis=0), wgate[1])) + 1.0
    update = gate * dot(tn, wout[1]) * jnp.concatenate(ms, axis=0)
    moved = jnp.concatenate(us, axis=0) + update
    part = ch // 2
    moved = pltpu.roll(moved, core * part, 1)[:, :part]
    out[...] = pair[...] + moved.reshape(tile_rows, tile_cols, part)


def swap_cores(x):
    return lax.ppermute(x, "gz", [(0, 1), (1, 0)])


def replicated(
    pair, residue_mask, norm_in_gain, proj_weight, gate_weight, norm_out_gain, out_weight
):
    part, tile_rows, tile_cols = pair.shape
    tile = jnp.transpose(pair, (1, 2, 0))
    grid_rows, grid_cols = lax.axis_size("gx"), lax.axis_size("gy")
    res = residue_mask.shape[0]
    ch = 2 * part
    half = tile_rows // 2
    ipad = -(-tile_rows // 8) * 8
    span = tile_cols + ipad

    other_tile = swap_cores(tile)
    chips = grid_rows * grid_cols
    message = pl.pallas_call(
        functools.partial(centre_kernel, half=half),
        out_shape=jax.ShapeDtypeStruct((chips, half * tile_cols, ch), BF16),
        compiler_params=pltpu.CompilerParams(vmem_limit_bytes=4 * 1024 * 1024),
        name="centre",
    )(tile, other_tile)
    own_weights = jnp.concatenate(
        [
            jnp.transpose(proj_weight, (0, 1, 3, 2)),
            jnp.transpose(gate_weight, (0, 2, 1))[:, None],
            jnp.transpose(out_weight, (0, 2, 1))[:, None],
        ],
        axis=1,
    )
    own_gains = jnp.concatenate([norm_in_gain, norm_out_gain], axis=0)
    gathered = lax.all_to_all(message, ("gx", "gy"), 0, 0)
    wleft, wright, wgate, wout, gains, mask = pl.pallas_call(
        weights_kernel,
        out_shape=[
            jax.ShapeDtypeStruct((2, ch, 2 * ch), BF16),
            jax.ShapeDtypeStruct((2, ch, 2 * ch), BF16),
            jax.ShapeDtypeStruct((2, ch, ch), BF16),
            jax.ShapeDtypeStruct((2, ch, ch), BF16),
            jax.ShapeDtypeStruct((4, ch), F32),
            jax.ShapeDtypeStruct((res + 8, ch), F32),
        ],
        compiler_params=pltpu.CompilerParams(vmem_limit_bytes=8 * 1024 * 1024),
        cost_estimate=pl.CostEstimate(flops=2**24, bytes_accessed=2**20, transcendentals=0),
        name="weights",
    )(own_weights, swap_cores(own_weights), own_gains, swap_cores(own_gains), residue_mask[None, :])
    other_gathered = swap_cores(gathered)

    def fitting(total, size):
        return size if total % size == 0 else next(n for n in (8, 4, 2, 1) if total % n == 0)

    sizes = {
        "norm": chips,
        "left": res,
        "right": fitting(tile_rows, 12) if tile_cols % 12 == 0 else 4,
        "tri": fitting(res, 4),
        "unroll": fitting(res, 24),
        "out": res,
        "second": res,
    }
    vmem = lambda rows: pltpu.VMEM((rows, ch), F32)
    result = pl.pallas_call(
        functools.partial(
            main_kernel,
            res=res,
            tile_rows=tile_rows,
            tile_cols=tile_cols,
            grid_rows=grid_rows,
            grid_cols=grid_cols,
            sizes=sizes,
        ),
        out_shape=jax.ShapeDtypeStruct(tile.shape, F32),
        scratch_shapes=[
            vmem(res * res + 8),
            vmem(res * res + 8),
            vmem(res * res),
            vmem(res * span),
            vmem(res * span),
            vmem(res * span),
            vmem(res * span),
            vmem(res * tile_cols),
            vmem(res * ipad),
        ],
        compiler_params=pltpu.CompilerParams(vmem_limit_bytes=24 * 1024 * 1024),
        name="update",
    )(gathered, other_gathered, mask, gains, wleft, wright, wgate, wout, tile)
    return jnp.transpose(result, (2, 0, 1))


def layer_norm_gathered(values, gain_part):
    full_values, full_gain = (
        lax.all_gather(values, "gz", axis=0, tiled=True),
        lax.all_gather(gain_part, "gz", axis=0, tiled=True),
    )
    mean_val = jnp.mean(full_values, axis=0)
    centred = full_values - mean_val
    spread = jnp.mean(centred * centred, axis=0)
    result = (centred * lax.rsqrt(spread + EPSILON) * full_gain[:, None, None]).astype(jnp.bfloat16)
    return result


def transpose_tile(pair_tile):
    depth_dim, tile_rows, tile_cols = pair_tile.shape
    across = lax.axis_size("gy")
    down_size = lax.axis_size("gx")
    quarter = tile_rows // across
    spread_rows = lax.all_to_all(pair_tile, "gy", split_axis=1, concat_axis=2, tiled=True)
    blocks = spread_rows.reshape(depth_dim, quarter, down_size, tile_rows)
    blocks = jnp.transpose(blocks, (0, 3, 2, 1))[:, :, :, None, :]
    moved_back = lax.all_to_all(
        lax.all_to_all(blocks, "gx", split_axis=2, concat_axis=2, tiled=True),
        "gy",
        split_axis=2,
        concat_axis=3,
        tiled=True,
    )
    return moved_back.reshape(depth_dim, tile_rows, tile_cols)


def fold_panels(left_tile, right_tile):
    left_panel = lax.all_gather(left_tile, "gy", axis=2, tiled=True)
    return jnp.einsum(
        "hik,hkj->hij",
        left_panel,
        lax.all_gather(right_tile, "gx", axis=1, tiled=True),
        preferred_element_type=jnp.float32,
    )


def distributed(
    pair, residue_mask, norm_in_gain, proj_weight, gate_weight, norm_out_gain, out_weight
):
    tile_rows = pair.shape[1]
    tile_cols = pair.shape[2]
    row_start = lax.axis_index("gx") * tile_rows
    col_start = lax.axis_index("gy") * tile_cols
    row_flags = lax.dynamic_slice_in_dim(residue_mask, row_start, tile_rows).astype(jnp.float32)
    col_flags = lax.dynamic_slice_in_dim(residue_mask, col_start, tile_cols).astype(jnp.float32)
    pair_mask = row_flags[:, None] * col_flags[None, :]
    current = pair
    for update in range(2):
        normed = layer_norm_gathered(current, norm_in_gain[update])
        projected = jnp.einsum(
            "cij,pch->phij", normed, proj_weight[update], preferred_element_type=jnp.float32
        )
        left_tile = (jax.nn.sigmoid(projected[0]) * projected[1] * pair_mask).astype(jnp.bfloat16)
        right_tile = (jax.nn.sigmoid(projected[2]) * projected[3] * pair_mask).astype(jnp.bfloat16)
        gate_values = jax.nn.sigmoid(
            jnp.einsum(
                "cij,cd->dij", normed, gate_weight[update], preferred_element_type=jnp.float32
            )
        )
        if update == 0:
            triangle = fold_panels(left_tile, transpose_tile(right_tile))
        else:
            triangle = fold_panels(transpose_tile(left_tile), right_tile)
        tri_normed = layer_norm_gathered(triangle, norm_out_gain[update])
        current = current + gate_values * jnp.einsum(
            "hij,hd->dij", tri_normed, out_weight[update], preferred_element_type=jnp.float32
        )
    return current


def fits_replicated(pair, residue_mask):
    part, tile_rows, tile_cols = pair.shape
    res = residue_mask.shape[0]
    return (
        lax.axis_size("gz") == 2
        and res * res * part * 2 * 4 <= REPLICATED_LIMIT
        and res % 8 == 0
        and tile_rows % 4 == 0
        and tile_cols % 8 == 0
    )


def per_device(pair, residue_mask, *parameters):
    plan = replicated if fits_replicated(pair, residue_mask) else distributed
    return plan(pair, residue_mask, *parameters)


def solution(mesh):
    return jax.shard_map(
        per_device,
        mesh=mesh,
        in_specs=(
            P(("groups", "gz"), "gx", "gy"),
            P("groups"),
            P(None, "gz"),
            P(None, None, None, "gz"),
            P(None, None, "gz"),
            P(None, "gz"),
            P(None, None, "gz"),
        ),
        out_specs=P(("groups", "gz"), "gx", "gy"),
        check_vma=False,
    )
```

```python
import functools

import jax
import jax.numpy as jnp
from jax import lax
from jax.experimental import pallas as pl
from jax.experimental.pallas import tpu as pltpu
from jax.sharding import PartitionSpec as P

EPSILON = 1e-05
F32 = jnp.float32
BF16 = jnp.bfloat16
REPLICATED_LIMIT = 4 * 1024 * 1024


def dot(x, w):
    return jnp.dot(x.astype(BF16), w, preferred_element_type=F32)


def lane_norm(x, gain, ones):
    d = x - jnp.mean(x, axis=-1, keepdims=True)
    return d * lax.rsqrt(dot(d * d, ones) + EPSILON) * gain


def gated(x, w):
    p = dot(x, w)
    ch = p.shape[1] // 2
    return (jnp.tanh(p[:, :ch]) + 1.0) * p[:, ch:]


def rows_at(first, count):
    return pl.ds(first if isinstance(first, int) else pl.multiple_of(first, 8), count)


def centre_kernel(own, other, out, *, half):
    core = lax.axis_index("gz")
    part = own.shape[2]
    pairs = half * own.shape[1]
    rows = pl.ds(core * half, half)
    both = jnp.concatenate(
        [own[rows].reshape(pairs, part), other[rows].reshape(pairs, part)], axis=1
    )
    both = pltpu.roll(both, core * part, 1)
    out[...] = (both - jnp.mean(both, axis=-1, keepdims=True)).astype(BF16)


def weights_kernel(own, other, own_gains, other_gains, flags, wleft, wright, wgate, wout, gains, mask):
    core = lax.axis_index("gz")
    half = own.shape[2]
    for u in range(2):
        for p in range(6):
            mine, theirs = own[u, p].astype(F32) * 0.5, other[u, p].astype(F32) * 0.5
            first = jnp.where(core == 0, mine, theirs)
            second = jnp.where(core == 0, theirs, mine)
            full = jnp.transpose(jnp.concatenate([first, second], axis=0)).astype(BF16)
            if p < 2:
                wleft[u, :, p * 2 * half : (p + 1) * 2 * half] = full
            elif p < 4:
                wright[u, :, (p - 2) * 2 * half : (p - 1) * 2 * half] = full
            elif p == 4:
                wgate[u] = full
            else:
                wout[u] = full
    gains[...] = pltpu.roll(jnp.concatenate([own_gains[...], other_gains[...]], axis=1), core * half, 1)
    row = flags[...].astype(F32)
    size = row.shape[1]
    wide = jnp.transpose(jnp.broadcast_to(row, (mask.shape[1], size)))
    mask[...] = jnp.zeros_like(mask)
    mask[:size, :] = wide


class Place:
    def __init__(self, res, tile_rows, tile_cols):
        self.res, self.rows, self.cols = res, tile_rows, tile_cols
        self.half = tile_rows // 2
        self.ipad = -(-tile_rows // 8) * 8
        self.span = tile_cols + self.ipad
        self.row_block = lax.axis_index("gx")
        self.col_block = lax.axis_index("gy")
        self.core = lax.axis_index("gz")
        self.first_row = self.row_block * tile_rows
        self.first_col = self.col_block * tile_cols


def column_phase(at, own, other, mask, gains, wleft, wright, raw, normed, left, rightt, tri, column, start):
    ch = mask.shape[1]
    cols, span = at.cols, at.span
    for s in range(own.shape[0]):
        for source, which in ((own, at.core), (other, 1 - at.core)):
            x = source[s].astype(F32)
            var = jnp.mean(x * x, axis=-1, keepdims=True)
            first = ((at.row_block ^ s) * at.rows + which * at.half) * cols
            where = pl.ds(pl.multiple_of(first, 8), at.half * cols)
            raw[where, :] = x
            normed[where, :] = x * lax.rsqrt(var + EPSILON) * gains[0:1, :]
    pairs = at.res * cols
    raw[pairs:, :] = jnp.zeros((raw.shape[0] - pairs, ch), F32)
    normed[pairs:, :] = jnp.zeros((raw.shape[0] - pairs, ch), F32)

    kmask = mask[rows_at(column * cols, cols), :]
    y = gated(normed[:pairs, :], wleft[0]).reshape(at.res, cols, ch) * kmask[None]
    left[...] = y.reshape(pairs, ch)

    for k in range(at.ipad - at.rows):
        rightt[pl.ds(cols + at.rows + k, cols, stride=span), :] = jnp.zeros((cols, ch), F32)
    for slot in range(0, cols + at.rows, at.rows):
        row = at.first_col + slot if slot < cols else at.first_row
        y = gated(normed[rows_at(row * cols, at.rows * cols), :], wright[0])
        for q in range(at.rows):
            rightt[pl.ds(slot + q, cols, stride=span), :] = y[q * cols : (q + 1) * cols]

    count = 4

    def tri_block(n, carry):
        first = n * count

        def add(k, accs):
            r = rightt[pl.ds(pl.multiple_of(k * span, 8), span), :]
            return tuple(acc + left[pl.ds((first + q) * cols + k, 1), :] * r for q, acc in enumerate(accs))

        where = [pl.ds(pl.multiple_of((first + q) * span, 8), span) for q in range(count)]
        accs = tuple(jnp.zeros((span, ch), F32) if start is None else start[w, :] for w in where)
        accs = lax.fori_loop(0, cols, add, accs, unroll=min(cols, 24))
        for w, acc in zip(where, accs):
            tri[w, :] = acc
        return carry

    lax.fori_loop(0, at.res // count, tri_block, 0)


def near_kernel(
    own, other, mask, gains, wleft, wright, raw, normed, tri, left, rightt, *, place
):
    at = Place(*place)
    column_phase(at, own, other, mask, gains, wleft, wright, raw, normed, left, rightt, tri, at.col_block, None)


def far_kernel(
    own, other, near_raw, near_normed, near_tri, mask, gains, wleft, wright, wgate, wout, pair, out,
    raw, normed, left, rightt, tri, first_update, znext, right1, left1, *, place,
):
    at = Place(*place)
    res, rows, cols, ipad, span = at.res, at.rows, at.cols, at.ipad, at.span
    ch = mask.shape[1]
    column_phase(
        at, own, other, mask, gains, wleft, wright, raw, normed, left, rightt, tri, 1 - at.col_block, near_tri
    )
    ones = jnp.full((ch, ch), 1.0 / ch, BF16)
    gain_in, gain_out = gains[0:2, :], gains[2:4, :]

    smask = jnp.concatenate(
        [mask[rows_at(at.first_col, cols), :], mask[pl.ds(at.first_row, ipad), :]], axis=0
    )
    row_is_near = at.first_row // cols == at.col_block
    offset = at.first_row % cols
    zs, ns, ms = [], [], []
    for r in range(res):
        where = pl.ds(r * cols + offset, ipad)
        zs += [near_raw[r * cols : (r + 1) * cols, :], jnp.where(row_is_near, near_raw[where, :], raw[where, :])]
        ns += [
            near_normed[r * cols : (r + 1) * cols, :],
            jnp.where(row_is_near, near_normed[where, :], normed[where, :]),
        ]
        ms.append(smask * mask[r : r + 1, :])
    gate = jnp.tanh(dot(jnp.concatenate(ns, axis=0), wgate[0])) + 1.0
    tn = lane_norm(tri[...], gain_out[0:1], ones)
    update = gate * dot(tn, wout[0]) * jnp.concatenate(ms, axis=0)
    first_update[...] = update
    znext[...] = lane_norm(jnp.concatenate(zs, axis=0) + update, gain_in[1:2], ones)

    z3 = znext[...].reshape(res, span, ch)
    right1[...] = gated(z3[:, :cols].reshape(res * cols, ch), wright[1])
    v = gated(z3[:, cols:].reshape(res * ipad, ch), wleft[1]).reshape(res, ipad, ch) * mask[:res, :][:, None, :]
    left1[...] = v.reshape(res * ipad, ch)

    def tri1_block(k, accs):
        r = right1[pl.ds(pl.multiple_of(k * cols, 8), cols), :]
        return tuple(acc + left1[pl.ds(k * ipad + i, 1), :] * r for i, acc in enumerate(accs))

    accs = lax.fori_loop(0, res, tri1_block, tuple(jnp.zeros((cols, ch), F32) for _ in range(rows)), unroll=4)
    tn = lane_norm(jnp.concatenate(accs, axis=0), gain_out[1:2], ones)
    ns, us, ms = [], [], []
    for i in range(rows):
        where = pl.ds(pl.multiple_of((at.first_row + i) * span, 8), cols)
        ns.append(znext[where, :])
        us.append(first_update[where, :])
        ms.append(smask[:cols] * mask[pl.ds(at.first_row + i, 1), :])
    gate = jnp.tanh(dot(jnp.concatenate(ns, axis=0), wgate[1])) + 1.0
    update = gate * dot(tn, wout[1]) * jnp.concatenate(ms, axis=0)
    moved = jnp.concatenate(us, axis=0) + update
    part = ch // 2
    moved = pltpu.roll(moved, at.core * part, 1)[:, :part]
    out[...] = pair[...] + moved.reshape(rows, cols, part)


def swap_cores(x):
    return lax.ppermute(x, "gz", [(0, 1), (1, 0)])


def replicated(
    pair, residue_mask, norm_in_gain, proj_weight, gate_weight, norm_out_gain, out_weight
):
    part, tile_rows, tile_cols = pair.shape
    tile = jnp.transpose(pair, (1, 2, 0))
    res = residue_mask.shape[0]
    ch = 2 * part
    half = tile_rows // 2
    ipad = -(-tile_rows // 8) * 8
    span = tile_cols + ipad
    other_tile = swap_cores(tile)
    message = pl.pallas_call(
        functools.partial(centre_kernel, half=half),
        out_shape=jax.ShapeDtypeStruct((half * tile_cols, ch), BF16),
        compiler_params=pltpu.CompilerParams(vmem_limit_bytes=4 * 1024 * 1024),
        name="centre",
    )(tile, other_tile)
    blocks = lax.axis_size("gx")
    column = jnp.stack(
        [message]
        + [lax.ppermute(message, "gx", [(i, i ^ s) for i in range(blocks)]) for s in range(1, blocks)]
    )
    far = lax.ppermute(column, "gy", [(0, 1), (1, 0)])
    own_weights = jnp.concatenate(
        [
            jnp.transpose(proj_weight, (0, 1, 3, 2)),
            jnp.transpose(gate_weight, (0, 2, 1))[:, None],
            jnp.transpose(out_weight, (0, 2, 1))[:, None],
        ],
        axis=1,
    )
    own_gains = jnp.concatenate([norm_in_gain, norm_out_gain], axis=0)
    wleft, wright, wgate, wout, gains, mask = pl.pallas_call(
        weights_kernel,
        out_shape=[
            jax.ShapeDtypeStruct((2, ch, 2 * ch), BF16),
            jax.ShapeDtypeStruct((2, ch, 2 * ch), BF16),
            jax.ShapeDtypeStruct((2, ch, ch), BF16),
            jax.ShapeDtypeStruct((2, ch, ch), BF16),
            jax.ShapeDtypeStruct((4, ch), F32),
            jax.ShapeDtypeStruct((res + 8, ch), F32),
        ],
        compiler_params=pltpu.CompilerParams(vmem_limit_bytes=8 * 1024 * 1024),
        cost_estimate=pl.CostEstimate(flops=2**24, bytes_accessed=2**20, transcendentals=0),
        name="weights",
    )(own_weights, swap_cores(own_weights), own_gains, swap_cores(own_gains), residue_mask[None, :])
    place = (res, tile_rows, tile_cols)
    pairs = res * tile_cols
    wide = lambda rows: jax.ShapeDtypeStruct((rows, ch), F32)
    vmem = lambda rows: pltpu.VMEM((rows, ch), F32)
    near_raw, near_normed, near_tri = pl.pallas_call(
        functools.partial(near_kernel, place=place),
        out_shape=[wide(pairs + 8), wide(pairs + 8), wide(res * span)],
        scratch_shapes=[vmem(pairs), vmem(tile_cols * span)],
        compiler_params=pltpu.CompilerParams(vmem_limit_bytes=12 * 1024 * 1024),
        cost_estimate=pl.CostEstimate(flops=2**28, bytes_accessed=2**21, transcendentals=0),
        name="near",
    )(column, swap_cores(column), mask, gains, wleft, wright)
    result = pl.pallas_call(
        functools.partial(far_kernel, place=place),
        out_shape=jax.ShapeDtypeStruct(tile.shape, F32),
        scratch_shapes=[
            vmem(pairs + 8),
            vmem(pairs + 8),
            vmem(pairs),
            vmem(tile_cols * span),
            vmem(res * span),
            vmem(res * span),
            vmem(res * span),
            vmem(pairs),
            vmem(res * ipad),
        ],
        compiler_params=pltpu.CompilerParams(vmem_limit_bytes=24 * 1024 * 1024),
        name="far",
    )(
        far, swap_cores(far), near_raw, near_normed, near_tri, mask, gains, wleft, wright, wgate, wout, tile,
    )
    return jnp.transpose(result, (2, 0, 1))


def layer_norm_gathered(values, gain_part):
    full_values, full_gain = (
        lax.all_gather(values, "gz", axis=0, tiled=True),
        lax.all_gather(gain_part, "gz", axis=0, tiled=True),
    )
    mean_val = jnp.mean(full_values, axis=0)
    centred = full_values - mean_val
    spread = jnp.mean(centred * centred, axis=0)
    result = (centred * lax.rsqrt(spread + EPSILON) * full_gain[:, None, None]).astype(jnp.bfloat16)
    return result


def transpose_tile(pair_tile):
    depth_dim, tile_rows, tile_cols = pair_tile.shape
    across = lax.axis_size("gy")
    down_size = lax.axis_size("gx")
    quarter = tile_rows // across
    spread_rows = lax.all_to_all(pair_tile, "gy", split_axis=1, concat_axis=2, tiled=True)
    blocks = spread_rows.reshape(depth_dim, quarter, down_size, tile_rows)
    blocks = jnp.transpose(blocks, (0, 3, 2, 1))[:, :, :, None, :]
    moved_back = lax.all_to_all(
        lax.all_to_all(blocks, "gx", split_axis=2, concat_axis=2, tiled=True),
        "gy",
        split_axis=2,
        concat_axis=3,
        tiled=True,
    )
    return moved_back.reshape(depth_dim, tile_rows, tile_cols)


def fold_panels(left_tile, right_tile):
    left_panel = lax.all_gather(left_tile, "gy", axis=2, tiled=True)
    return jnp.einsum(
        "hik,hkj->hij",
        left_panel,
        lax.all_gather(right_tile, "gx", axis=1, tiled=True),
        preferred_element_type=jnp.float32,
    )


def distributed(
    pair, residue_mask, norm_in_gain, proj_weight, gate_weight, norm_out_gain, out_weight
):
    tile_rows = pair.shape[1]
    tile_cols = pair.shape[2]
    row_start = lax.axis_index("gx") * tile_rows
    col_start = lax.axis_index("gy") * tile_cols
    row_flags = lax.dynamic_slice_in_dim(residue_mask, row_start, tile_rows).astype(jnp.float32)
    col_flags = lax.dynamic_slice_in_dim(residue_mask, col_start, tile_cols).astype(jnp.float32)
    pair_mask = row_flags[:, None] * col_flags[None, :]
    current = pair
    for update in range(2):
        normed = layer_norm_gathered(current, norm_in_gain[update])
        projected = jnp.einsum(
            "cij,pch->phij", normed, proj_weight[update], preferred_element_type=jnp.float32
        )
        left_tile = (jax.nn.sigmoid(projected[0]) * projected[1] * pair_mask).astype(jnp.bfloat16)
        right_tile = (jax.nn.sigmoid(projected[2]) * projected[3] * pair_mask).astype(jnp.bfloat16)
        gate_values = jax.nn.sigmoid(
            jnp.einsum(
                "cij,cd->dij", normed, gate_weight[update], preferred_element_type=jnp.float32
            )
        )
        if update == 0:
            triangle = fold_panels(left_tile, transpose_tile(right_tile))
        else:
            triangle = fold_panels(transpose_tile(left_tile), right_tile)
        tri_normed = layer_norm_gathered(triangle, norm_out_gain[update])
        current = current + gate_values * jnp.einsum(
            "hij,hd->dij", tri_normed, out_weight[update], preferred_element_type=jnp.float32
        )
    return current


def fits_replicated(pair, residue_mask):
    part, tile_rows, tile_cols = pair.shape
    res = residue_mask.shape[0]
    return (
        lax.axis_size("gz") == 2
        and res * res * part * 2 * 4 <= REPLICATED_LIMIT
        and lax.axis_size("gy") == 2
        and lax.axis_size("gx").bit_count() == 1
        and res % 4 == 0
        and tile_rows % 2 == 0
        and tile_cols % 8 == 0
        and tile_cols % tile_rows == 0
    )


def per_device(pair, residue_mask, *parameters):
    plan = replicated if fits_replicated(pair, residue_mask) else distributed
    return plan(pair, residue_mask, *parameters)


def solution(mesh):
    return jax.shard_map(
        per_device,
        mesh=mesh,
        in_specs=(
            P(("groups", "gz"), "gx", "gy"),
            P("groups"),
            P(None, "gz"),
            P(None, None, None, "gz"),
            P(None, None, "gz"),
            P(None, "gz"),
            P(None, None, "gz"),
        ),
        out_specs=P(("groups", "gz"), "gx", "gy"),
        check_vma=False,
    )
```

```python
import functools

import jax
import jax.numpy as jnp
from jax import lax
from jax.experimental import pallas as pl
from jax.experimental.pallas import tpu as pltpu
from jax.sharding import PartitionSpec as P


EPSILON = 1e-05
F32 = jnp.float32
BF16 = jnp.bfloat16
REPLICATED_LIMIT = 4 * 1024 * 1024


def dot(x, w):
    return jnp.dot(x.astype(BF16), w, preferred_element_type=F32)


def lane_norm(x, gain, ones):
    d = x - jnp.mean(x, axis=-1, keepdims=True)
    return d * lax.rsqrt(dot(d * d, ones) + EPSILON) * gain


def gated(x, w):
    p = dot(x, w)
    ch = p.shape[1] // 2
    return (jnp.tanh(p[:, :ch]) + 1.0) * p[:, ch:]


def rows_at(first, count):
    return pl.ds(first if isinstance(first, int) else pl.multiple_of(first, 8), count)


def own_kernel(tile, out):
    half = tile.shape[0] // 2
    rows = tile[pl.ds(lax.axis_index("gz") * half, half)]
    out[...] = rows.reshape(out.shape)


def centre_kernel(own, other, out):
    core = lax.axis_index("gz")
    pairs, part = own.shape
    half = other.shape[0] // 2
    theirs = other[pl.ds(core * half, half)].reshape(pairs, part)
    both = pltpu.roll(jnp.concatenate([own[...], theirs], axis=1), core * part, 1)
    out[...] = (both - jnp.mean(both, axis=-1, keepdims=True)).astype(BF16)


def weights_kernel(own, other, own_gains, other_gains, flags, wleft, wright, wgate, wout, gains, mask):
    core = lax.axis_index("gz")
    half = own.shape[2]
    for u in range(2):
        for p in range(6):
            mine, theirs = own[u, p].astype(F32) * 0.5, other[u, p].astype(F32) * 0.5
            first = jnp.where(core == 0, mine, theirs)
            second = jnp.where(core == 0, theirs, mine)
            full = jnp.transpose(jnp.concatenate([first, second], axis=0)).astype(BF16)
            if p < 2:
                wleft[u, :, p * 2 * half : (p + 1) * 2 * half] = full
            elif p < 4:
                wright[u, :, (p - 2) * 2 * half : (p - 1) * 2 * half] = full
            elif p == 4:
                wgate[u] = full
            else:
                wout[u] = full
    gains[...] = pltpu.roll(jnp.concatenate([own_gains[...], other_gains[...]], axis=1), core * half, 1)
    row = flags[...].astype(F32)
    size = row.shape[1]
    wide = jnp.transpose(jnp.broadcast_to(row, (mask.shape[1], size)))
    mask[...] = jnp.zeros_like(mask)
    mask[:size, :] = wide


class Place:
    def __init__(self, res, tile_rows, tile_cols):
        self.res, self.rows, self.cols = res, tile_rows, tile_cols
        self.half = tile_rows // 2
        self.ipad = -(-tile_rows // 8) * 8
        self.span = tile_cols + self.ipad
        self.row_block = lax.axis_index("gx")
        self.col_block = lax.axis_index("gy")
        self.core = lax.axis_index("gz")
        self.first_row = self.row_block * tile_rows
        self.first_col = self.col_block * tile_cols


def column_phase(at, own, other, mask, gains, wleft, wright, raw, normed, left, rightt, column):
    ch = mask.shape[1]
    cols, span = at.cols, at.span
    for s in range(own.shape[0]):
        for source, which in ((own, at.core), (other, 1 - at.core)):
            x = source[s].astype(F32)
            var = jnp.mean(x * x, axis=-1, keepdims=True)
            first = ((at.row_block ^ s) * at.rows + which * at.half) * cols
            where = pl.ds(pl.multiple_of(first, 8), at.half * cols)
            raw[where, :] = x
            normed[where, :] = x * lax.rsqrt(var + EPSILON) * gains[0:1, :]
    pairs = at.res * cols
    raw[pairs:, :] = jnp.zeros((raw.shape[0] - pairs, ch), F32)
    normed[pairs:, :] = jnp.zeros((raw.shape[0] - pairs, ch), F32)

    kmask = mask[rows_at(column * cols, cols), :]
    y = gated(normed[:pairs, :], wleft[0]).reshape(at.res, cols, ch) * kmask[None]
    left[...] = y.reshape(pairs, ch)

    for k in range(at.ipad - at.rows):
        rightt[pl.ds(cols + at.rows + k, cols, stride=span), :] = jnp.zeros((cols, ch), F32)
    for slot in range(0, cols + at.rows, at.rows):
        row = at.first_col + slot if slot < cols else at.first_row
        y = gated(normed[rows_at(row * cols, at.rows * cols), :], wright[0])
        for q in range(at.rows):
            rightt[pl.ds(slot + q, cols, stride=span), :] = y[q * cols : (q + 1) * cols]


def triangle_phase(at, left, rightt, tri, start):
    cols, span = at.cols, at.span
    ch = left.shape[1]
    count = 4

    def tri_block(n, carry):
        first = n * count

        def add(k, accs):
            r = rightt[pl.ds(pl.multiple_of(k * span, 8), span), :]
            return tuple(acc + left[pl.ds((first + q) * cols + k, 1), :] * r for q, acc in enumerate(accs))

        where = [pl.ds(pl.multiple_of((first + q) * span, 8), span) for q in range(count)]
        accs = tuple(jnp.zeros((span, ch), F32) if start is None else start[w, :] for w in where)
        accs = lax.fori_loop(0, cols, add, accs, unroll=min(cols, 24))
        for w, acc in zip(where, accs):
            tri[w, :] = acc
        return carry

    lax.fori_loop(0, at.res // count, tri_block, 0)


def near_kernel(own, other, mask, gains, wleft, wright, raw, normed, left, rightt, *, place):
    at = Place(*place)
    column_phase(at, own, other, mask, gains, wleft, wright, raw, normed, left, rightt, at.col_block)


def near_triangle_kernel(left, rightt, tri, *, place):
    triangle_phase(Place(*place), left, rightt, tri, None)


def far_kernel(
    own, other, near_raw, near_normed, near_tri, mask, gains, wleft, wright, wgate, wout, pair, out,
    raw, normed, left, rightt, tri, first_update, znext, right1, left1, *, place,
):
    at = Place(*place)
    res, rows, cols, ipad, span = at.res, at.rows, at.cols, at.ipad, at.span
    ch = mask.shape[1]
    column_phase(at, own, other, mask, gains, wleft, wright, raw, normed, left, rightt, 1 - at.col_block)
    triangle_phase(at, left, rightt, tri, near_tri)
    ones = jnp.full((ch, ch), 1.0 / ch, BF16)
    gain_in, gain_out = gains[0:2, :], gains[2:4, :]

    smask = jnp.concatenate(
        [mask[rows_at(at.first_col, cols), :], mask[pl.ds(at.first_row, ipad), :]], axis=0
    )
    row_is_near = at.first_row // cols == at.col_block
    offset = at.first_row % cols
    zs, ns, ms = [], [], []
    for r in range(res):
        where = pl.ds(r * cols + offset, ipad)
        zs += [near_raw[r * cols : (r + 1) * cols, :], jnp.where(row_is_near, near_raw[where, :], raw[where, :])]
        ns += [
            near_normed[r * cols : (r + 1) * cols, :],
            jnp.where(row_is_near, near_normed[where, :], normed[where, :]),
        ]
        ms.append(smask * mask[r : r + 1, :])
    gate = jnp.tanh(dot(jnp.concatenate(ns, axis=0), wgate[0])) + 1.0
    tn = lane_norm(tri[...], gain_out[0:1], ones)
    update = gate * dot(tn, wout[0]) * jnp.concatenate(ms, axis=0)
    first_update[...] = update
    znext[...] = lane_norm(jnp.concatenate(zs, axis=0) + update, gain_in[1:2], ones)

    z3 = znext[...].reshape(res, span, ch)
    right1[...] = gated(z3[:, :cols].reshape(res * cols, ch), wright[1])
    v = gated(z3[:, cols:].reshape(res * ipad, ch), wleft[1]).reshape(res, ipad, ch) * mask[:res, :][:, None, :]
    left1[...] = v.reshape(res * ipad, ch)

    def tri1_block(k, accs):
        r = right1[pl.ds(pl.multiple_of(k * cols, 8), cols), :]
        return tuple(acc + left1[pl.ds(k * ipad + i, 1), :] * r for i, acc in enumerate(accs))

    accs = lax.fori_loop(0, res, tri1_block, tuple(jnp.zeros((cols, ch), F32) for _ in range(rows)), unroll=4)
    tn = lane_norm(jnp.concatenate(accs, axis=0), gain_out[1:2], ones)
    ns, us, ms = [], [], []
    for i in range(rows):
        where = pl.ds(pl.multiple_of((at.first_row + i) * span, 8), cols)
        ns.append(znext[where, :])
        us.append(first_update[where, :])
        ms.append(smask[:cols] * mask[pl.ds(at.first_row + i, 1), :])
    gate = jnp.tanh(dot(jnp.concatenate(ns, axis=0), wgate[1])) + 1.0
    update = gate * dot(tn, wout[1]) * jnp.concatenate(ms, axis=0)
    moved = jnp.concatenate(us, axis=0) + update
    part = ch // 2
    moved = pltpu.roll(moved, at.core * part, 1)[:, :part]
    out[...] = pair[...] + moved.reshape(rows, cols, part)


def swap(x, axis, mask=1):
    size = lax.axis_size(axis)
    return lax.ppermute(x, axis, [(i, i ^ mask) for i in range(size)])


def call(kernel, out_shape, *args, scratch=(), vmem_mib=4, flops=2**20):
    return pl.pallas_call(
        kernel,
        out_shape=out_shape,
        scratch_shapes=list(scratch),
        compiler_params=pltpu.CompilerParams(vmem_limit_bytes=vmem_mib * 1024 * 1024),
        cost_estimate=pl.CostEstimate(flops=flops, bytes_accessed=2**16, transcendentals=0),
    )(*args)


def replicated(
    pair, residue_mask, norm_in_gain, proj_weight, gate_weight, norm_out_gain, out_weight
):
    part, tile_rows, tile_cols = pair.shape
    tile = jnp.transpose(pair, (1, 2, 0))
    res = residue_mask.shape[0]
    ch = 2 * part
    half = tile_rows // 2
    ipad = -(-tile_rows // 8) * 8
    span = tile_cols + ipad
    blocks = lax.axis_size("gx")
    place = (res, tile_rows, tile_cols)
    pairs = res * tile_cols
    wide = lambda rows: jax.ShapeDtypeStruct((rows, ch), F32)
    vmem = lambda rows: pltpu.VMEM((rows, ch), F32)
    narrow = lambda *shape: jax.ShapeDtypeStruct(shape, BF16)

    other_tile = swap(tile, "gz")
    own_weights = jnp.concatenate(
        [
            jnp.transpose(proj_weight, (0, 1, 3, 2)),
            jnp.transpose(gate_weight, (0, 2, 1))[:, None],
            jnp.transpose(out_weight, (0, 2, 1))[:, None],
        ],
        axis=1,
    )
    own_gains = jnp.concatenate([norm_in_gain, norm_out_gain], axis=0)
    other_weights = swap(own_weights, "gz")
    other_gains = swap(own_gains, "gz")

    own_rows = call(own_kernel, jax.ShapeDtypeStruct((half * tile_cols, part), F32), tile)
    message = call(centre_kernel, narrow(half * tile_cols, ch), own_rows, other_tile)
    column = [message]
    for s in range(1, blocks):
        column.append(swap(message, "gx", s))
    wleft, wright, wgate, wout, gains, mask = call(
        weights_kernel,
        [narrow(2, ch, 2 * ch), narrow(2, ch, 2 * ch), narrow(2, ch, ch), narrow(2, ch, ch), wide(4), wide(res + 8)],
        own_weights, other_weights, own_gains, other_gains, residue_mask[None, :],
        vmem_mib=8,
    )
    near = jnp.stack(column)
    far = swap(near, "gy")
    near_other = swap(near, "gz")
    far_other = swap(far, "gz")
    near_raw, near_normed, near_left, near_right = call(
        functools.partial(near_kernel, place=place),
        [wide(pairs + 8), wide(pairs + 8), wide(pairs), wide(tile_cols * span)],
        near, near_other, mask, gains, wleft, wright,
        flops=2**26,
    )
    near_tri = call(
        functools.partial(near_triangle_kernel, place=place),
        wide(res * span),
        near_left, near_right,
        flops=2**26,
    )
    result = call(
        functools.partial(far_kernel, place=place),
        jax.ShapeDtypeStruct(tile.shape, F32),
        far, far_other, near_raw, near_normed, near_tri, mask, gains, wleft, wright, wgate, wout, tile,
        scratch=[
            vmem(pairs + 8),
            vmem(pairs + 8),
            vmem(pairs),
            vmem(tile_cols * span),
            vmem(res * span),
            vmem(res * span),
            vmem(res * span),
            vmem(pairs),
            vmem(res * ipad),
        ],
        vmem_mib=24,
    )
    return jnp.transpose(result, (2, 0, 1))


def layer_norm_gathered(values, gain_part):
    full_values, full_gain = (
        lax.all_gather(values, "gz", axis=0, tiled=True),
        lax.all_gather(gain_part, "gz", axis=0, tiled=True),
    )
    mean_val = jnp.mean(full_values, axis=0)
    centred = full_values - mean_val
    spread = jnp.mean(centred * centred, axis=0)
    result = (centred * lax.rsqrt(spread + EPSILON) * full_gain[:, None, None]).astype(jnp.bfloat16)
    return result


def transpose_tile(pair_tile):
    depth_dim, tile_rows, tile_cols = pair_tile.shape
    across = lax.axis_size("gy")
    down_size = lax.axis_size("gx")
    quarter = tile_rows // across
    spread_rows = lax.all_to_all(pair_tile, "gy", split_axis=1, concat_axis=2, tiled=True)
    blocks = spread_rows.reshape(depth_dim, quarter, down_size, tile_rows)
    blocks = jnp.transpose(blocks, (0, 3, 2, 1))[:, :, :, None, :]
    moved_back = lax.all_to_all(
        lax.all_to_all(blocks, "gx", split_axis=2, concat_axis=2, tiled=True),
        "gy",
        split_axis=2,
        concat_axis=3,
        tiled=True,
    )
    return moved_back.reshape(depth_dim, tile_rows, tile_cols)


def fold_panels(left_tile, right_tile):
    left_panel = lax.all_gather(left_tile, "gy", axis=2, tiled=True)
    return jnp.einsum(
        "hik,hkj->hij",
        left_panel,
        lax.all_gather(right_tile, "gx", axis=1, tiled=True),
        preferred_element_type=jnp.float32,
    )


def distributed(
    pair, residue_mask, norm_in_gain, proj_weight, gate_weight, norm_out_gain, out_weight
):
    tile_rows = pair.shape[1]
    tile_cols = pair.shape[2]
    row_start = lax.axis_index("gx") * tile_rows
    col_start = lax.axis_index("gy") * tile_cols
    row_flags = lax.dynamic_slice_in_dim(residue_mask, row_start, tile_rows).astype(jnp.float32)
    col_flags = lax.dynamic_slice_in_dim(residue_mask, col_start, tile_cols).astype(jnp.float32)
    pair_mask = row_flags[:, None] * col_flags[None, :]
    current = pair
    for update in range(2):
        normed = layer_norm_gathered(current, norm_in_gain[update])
        projected = jnp.einsum(
            "cij,pch->phij", normed, proj_weight[update], preferred_element_type=jnp.float32
        )
        left_tile = (jax.nn.sigmoid(projected[0]) * projected[1] * pair_mask).astype(jnp.bfloat16)
        right_tile = (jax.nn.sigmoid(projected[2]) * projected[3] * pair_mask).astype(jnp.bfloat16)
        gate_values = jax.nn.sigmoid(
            jnp.einsum(
                "cij,cd->dij", normed, gate_weight[update], preferred_element_type=jnp.float32
            )
        )
        if update == 0:
            triangle = fold_panels(left_tile, transpose_tile(right_tile))
        else:
            triangle = fold_panels(transpose_tile(left_tile), right_tile)
        tri_normed = layer_norm_gathered(triangle, norm_out_gain[update])
        current = current + gate_values * jnp.einsum(
            "hij,hd->dij", tri_normed, out_weight[update], preferred_element_type=jnp.float32
        )
    return current


def fits_replicated(pair, residue_mask):
    part, tile_rows, tile_cols = pair.shape
    res = residue_mask.shape[0]
    return (
        lax.axis_size("gz") == 2
        and res * res * part * 2 * 4 <= REPLICATED_LIMIT
        and lax.axis_size("gy") == 2
        and lax.axis_size("gx").bit_count() == 1
        and res % 4 == 0
        and tile_rows % 2 == 0
        and tile_cols % 8 == 0
        and tile_cols % tile_rows == 0
    )


def per_device(pair, residue_mask, *parameters):
    plan = replicated if fits_replicated(pair, residue_mask) else distributed
    return plan(pair, residue_mask, *parameters)


def solution(mesh):
    return jax.shard_map(
        per_device,
        mesh=mesh,
        in_specs=(
            P(("groups", "gz"), "gx", "gy"),
            P("groups"),
            P(None, "gz"),
            P(None, None, None, "gz"),
            P(None, None, "gz"),
            P(None, "gz"),
            P(None, None, "gz"),
        ),
        out_specs=P(("groups", "gz"), "gx", "gy"),
        check_vma=False,
    )
```

```python
import functools

import jax
import jax.numpy as jnp
from jax import lax
from jax.experimental import pallas as pl
from jax.experimental.pallas import tpu as pltpu
from jax.sharding import PartitionSpec as P


EPSILON = 1e-05
F32 = jnp.float32
BF16 = jnp.bfloat16
REPLICATED_LIMIT = 4 * 1024 * 1024


def dot(x, w):
    return jnp.dot(x.astype(BF16), w, preferred_element_type=F32)


def lane_norm(x, gain, ones):
    d = x - jnp.mean(x, axis=-1, keepdims=True)
    return d * lax.rsqrt(dot(d * d, ones) + EPSILON) * gain


def gated(x, w):
    p = dot(x, w)
    ch = p.shape[1] // 2
    return (jnp.tanh(p[:, :ch]) + 1.0) * p[:, ch:]


def rows_at(first, count):
    return pl.ds(first if isinstance(first, int) else pl.multiple_of(first, 8), count)


def own_kernel(tile, out, whole):
    half = tile.shape[0] // 2
    rows = tile[pl.ds(lax.axis_index("gz") * half, half)]
    out[...] = rows.reshape(out.shape)
    whole[...] = tile[...]


def centre_kernel(own, other, out):
    core = lax.axis_index("gz")
    pairs, part = own.shape
    half = other.shape[0] // 2
    theirs = other[pl.ds(core * half, half)].reshape(pairs, part)
    both = pltpu.roll(jnp.concatenate([own[...], theirs], axis=1), core * part, 1)
    out[...] = (both - jnp.mean(both, axis=-1, keepdims=True)).astype(BF16)


def weights_kernel(own, other, own_gains, other_gains, flags, wleft, wright, wgate, wout, gains, mask):
    core = lax.axis_index("gz")
    half = own.shape[2]
    for u in range(2):
        for p in range(6):
            mine, theirs = own[u, p].astype(F32) * 0.5, other[u, p].astype(F32) * 0.5
            first = jnp.where(core == 0, mine, theirs)
            second = jnp.where(core == 0, theirs, mine)
            full = jnp.transpose(jnp.concatenate([first, second], axis=0)).astype(BF16)
            if p < 2:
                wleft[u, :, p * 2 * half : (p + 1) * 2 * half] = full
            elif p < 4:
                wright[u, :, (p - 2) * 2 * half : (p - 1) * 2 * half] = full
            elif p == 4:
                wgate[u] = full
            else:
                wout[u] = full
    gains[...] = pltpu.roll(jnp.concatenate([own_gains[...], other_gains[...]], axis=1), core * half, 1)
    row = flags[...].astype(F32)
    size = row.shape[1]
    wide = jnp.transpose(jnp.broadcast_to(row, (mask.shape[1], size)))
    mask[...] = jnp.zeros_like(mask)
    mask[:size, :] = wide


class Place:
    def __init__(self, res, tile_rows, tile_cols):
        self.res, self.rows, self.cols = res, tile_rows, tile_cols
        self.half = tile_rows // 2
        self.ipad = -(-tile_rows // 8) * 8
        self.span = tile_cols + self.ipad
        self.row_block = lax.axis_index("gx")
        self.col_block = lax.axis_index("gy")
        self.core = lax.axis_index("gz")
        self.first_row = self.row_block * tile_rows
        self.first_col = self.col_block * tile_cols


def column_phase(at, own, other, mask, gains, wleft, wright, raw, normed, left, rightt, column):
    ch = mask.shape[1]
    cols, span = at.cols, at.span
    for s in range(own.shape[0]):
        for source, which in ((own, at.core), (other, 1 - at.core)):
            x = source[s].astype(F32)
            var = jnp.mean(x * x, axis=-1, keepdims=True)
            first = ((at.row_block ^ s) * at.rows + which * at.half) * cols
            where = pl.ds(pl.multiple_of(first, 8), at.half * cols)
            raw[where, :] = x
            normed[where, :] = x * lax.rsqrt(var + EPSILON) * gains[0:1, :]
    pairs = at.res * cols
    raw[pairs:, :] = jnp.zeros((raw.shape[0] - pairs, ch), F32)
    normed[pairs:, :] = jnp.zeros((raw.shape[0] - pairs, ch), F32)

    kmask = mask[rows_at(column * cols, cols), :]
    y = gated(normed[:pairs, :], wleft[0]).reshape(at.res, cols, ch) * kmask[None]
    left[...] = y.reshape(pairs, ch)

    for k in range(at.ipad - at.rows):
        rightt[pl.ds(cols + at.rows + k, cols, stride=span), :] = jnp.zeros((cols, ch), F32)
    for slot in range(0, cols + at.rows, at.rows):
        row = at.first_col + slot if slot < cols else at.first_row
        y = gated(normed[rows_at(row * cols, at.rows * cols), :], wright[0])
        for q in range(at.rows):
            rightt[pl.ds(slot + q, cols, stride=span), :] = y[q * cols : (q + 1) * cols]


def triangle_phase(at, left, rightt, tri, start):
    cols, span = at.cols, at.span
    ch = left.shape[1]
    count = 4

    def tri_block(n, carry):
        first = n * count

        def add(k, accs):
            r = rightt[pl.ds(pl.multiple_of(k * span, 8), span), :]
            return tuple(acc + left[pl.ds((first + q) * cols + k, 1), :] * r for q, acc in enumerate(accs))

        where = [pl.ds(pl.multiple_of((first + q) * span, 8), span) for q in range(count)]
        accs = tuple(jnp.zeros((span, ch), F32) if start is None else start[w, :] for w in where)
        accs = lax.fori_loop(0, cols, add, accs, unroll=min(cols, 24))
        for w, acc in zip(where, accs):
            tri[w, :] = acc
        return carry

    lax.fori_loop(0, at.res // count, tri_block, 0)


def near_kernel(own, other, mask, gains, wleft, wright, raw, normed, left, rightt, *, place):
    at = Place(*place)
    column_phase(at, own, other, mask, gains, wleft, wright, raw, normed, left, rightt, at.col_block)


def near_triangle_kernel(left, rightt, tri, *, place):
    triangle_phase(Place(*place), left, rightt, tri, None)


def far_kernel(
    own, other, near_raw, near_normed, near_tri, mask, gains, wleft, wright, wgate, wout, pair, out,
    raw, normed, left, rightt, tri, first_update, znext, right1, left1, *, place,
):
    at = Place(*place)
    res, rows, cols, ipad, span = at.res, at.rows, at.cols, at.ipad, at.span
    ch = mask.shape[1]
    column_phase(at, own, other, mask, gains, wleft, wright, raw, normed, left, rightt, 1 - at.col_block)
    triangle_phase(at, left, rightt, tri, near_tri)
    ones = jnp.full((ch, ch), 1.0 / ch, BF16)
    gain_in, gain_out = gains[0:2, :], gains[2:4, :]

    smask = jnp.concatenate(
        [mask[rows_at(at.first_col, cols), :], mask[pl.ds(at.first_row, ipad), :]], axis=0
    )
    row_is_near = at.first_row // cols == at.col_block
    offset = at.first_row % cols
    zs, ns, ms = [], [], []
    for r in range(res):
        where = pl.ds(r * cols + offset, ipad)
        zs += [near_raw[r * cols : (r + 1) * cols, :], jnp.where(row_is_near, near_raw[where, :], raw[where, :])]
        ns += [
            near_normed[r * cols : (r + 1) * cols, :],
            jnp.where(row_is_near, near_normed[where, :], normed[where, :]),
        ]
        ms.append(smask * mask[r : r + 1, :])
    gate = jnp.tanh(dot(jnp.concatenate(ns, axis=0), wgate[0])) + 1.0
    tn = lane_norm(tri[...], gain_out[0:1], ones)
    update = gate * dot(tn, wout[0]) * jnp.concatenate(ms, axis=0)
    first_update[...] = update
    znext[...] = lane_norm(jnp.concatenate(zs, axis=0) + update, gain_in[1:2], ones)

    z3 = znext[...].reshape(res, span, ch)
    right1[...] = gated(z3[:, :cols].reshape(res * cols, ch), wright[1])
    v = gated(z3[:, cols:].reshape(res * ipad, ch), wleft[1]).reshape(res, ipad, ch) * mask[:res, :][:, None, :]
    left1[...] = v.reshape(res * ipad, ch)

    def tri1_block(k, accs):
        r = right1[pl.ds(pl.multiple_of(k * cols, 8), cols), :]
        return tuple(acc + left1[pl.ds(k * ipad + i, 1), :] * r for i, acc in enumerate(accs))

    accs = lax.fori_loop(0, res, tri1_block, tuple(jnp.zeros((cols, ch), F32) for _ in range(rows)), unroll=4)
    tn = lane_norm(jnp.concatenate(accs, axis=0), gain_out[1:2], ones)
    ns, us, ms = [], [], []
    for i in range(rows):
        where = pl.ds(pl.multiple_of((at.first_row + i) * span, 8), cols)
        ns.append(znext[where, :])
        us.append(first_update[where, :])
        ms.append(smask[:cols] * mask[pl.ds(at.first_row + i, 1), :])
    gate = jnp.tanh(dot(jnp.concatenate(ns, axis=0), wgate[1])) + 1.0
    update = gate * dot(tn, wout[1]) * jnp.concatenate(ms, axis=0)
    moved = jnp.concatenate(us, axis=0) + update
    part = ch // 2
    moved = pltpu.roll(moved, at.core * part, 1)[:, :part]
    out[...] = pair[...] + moved.reshape(rows, cols, part)


def swap(x, axis, mask=1):
    size = lax.axis_size(axis)
    return lax.ppermute(x, axis, [(i, i ^ mask) for i in range(size)])


def call(kernel, out_shape, *args, scratch=(), vmem_mib=4, flops=2**20):
    return pl.pallas_call(
        kernel,
        out_shape=out_shape,
        scratch_shapes=list(scratch),
        compiler_params=pltpu.CompilerParams(vmem_limit_bytes=vmem_mib * 1024 * 1024),
        cost_estimate=pl.CostEstimate(flops=flops, bytes_accessed=2**16, transcendentals=0),
    )(*args)


def replicated(
    pair, residue_mask, norm_in_gain, proj_weight, gate_weight, norm_out_gain, out_weight
):
    part, tile_rows, tile_cols = pair.shape
    tile = jnp.transpose(pair, (1, 2, 0))
    res = residue_mask.shape[0]
    ch = 2 * part
    half = tile_rows // 2
    ipad = -(-tile_rows // 8) * 8
    span = tile_cols + ipad
    blocks = lax.axis_size("gx")
    place = (res, tile_rows, tile_cols)
    pairs = res * tile_cols
    wide = lambda rows: jax.ShapeDtypeStruct((rows, ch), F32)
    vmem = lambda rows: pltpu.VMEM((rows, ch), F32)
    narrow = lambda *shape: jax.ShapeDtypeStruct(shape, BF16)

    other_tile = swap(tile, "gz")
    own_weights = jnp.concatenate(
        [
            jnp.transpose(proj_weight, (0, 1, 3, 2)),
            jnp.transpose(gate_weight, (0, 2, 1))[:, None],
            jnp.transpose(out_weight, (0, 2, 1))[:, None],
        ],
        axis=1,
    )
    own_gains = jnp.concatenate([norm_in_gain, norm_out_gain], axis=0)
    other_weights = swap(own_weights, "gz")
    other_gains = swap(own_gains, "gz")

    own_rows, kept_tile = call(
        own_kernel, [jax.ShapeDtypeStruct((half * tile_cols, part), F32), jax.ShapeDtypeStruct(tile.shape, F32)], tile
    )
    message = call(centre_kernel, narrow(half * tile_cols, ch), own_rows, other_tile)
    column = [message]
    for s in range(1, blocks):
        column.append(swap(message, "gx", s))
    wleft, wright, wgate, wout, gains, mask = call(
        weights_kernel,
        [narrow(2, ch, 2 * ch), narrow(2, ch, 2 * ch), narrow(2, ch, ch), narrow(2, ch, ch), wide(4), wide(res + 8)],
        own_weights, other_weights, own_gains, other_gains, residue_mask[None, :],
        vmem_mib=8,
    )
    near = jnp.stack(column)
    far = swap(near, "gy")
    near_other = swap(near, "gz")
    far_other = swap(far, "gz")
    near_raw, near_normed, near_left, near_right = call(
        functools.partial(near_kernel, place=place),
        [wide(pairs + 8), wide(pairs + 8), wide(pairs), wide(tile_cols * span)],
        near, near_other, mask, gains, wleft, wright,
        flops=2**26,
    )
    near_tri = call(
        functools.partial(near_triangle_kernel, place=place),
        wide(res * span),
        near_left, near_right,
        flops=2**26,
    )
    result = call(
        functools.partial(far_kernel, place=place),
        jax.ShapeDtypeStruct(tile.shape, F32),
        far, far_other, near_raw, near_normed, near_tri, mask, gains, wleft, wright, wgate, wout, kept_tile,
        scratch=[
            vmem(pairs + 8),
            vmem(pairs + 8),
            vmem(pairs),
            vmem(tile_cols * span),
            vmem(res * span),
            vmem(res * span),
            vmem(res * span),
            vmem(pairs),
            vmem(res * ipad),
        ],
        vmem_mib=24,
    )
    return jnp.transpose(result, (2, 0, 1))


def layer_norm_gathered(values, gain_part):
    full_values, full_gain = (
        lax.all_gather(values, "gz", axis=0, tiled=True),
        lax.all_gather(gain_part, "gz", axis=0, tiled=True),
    )
    mean_val = jnp.mean(full_values, axis=0)
    centred = full_values - mean_val
    spread = jnp.mean(centred * centred, axis=0)
    result = (centred * lax.rsqrt(spread + EPSILON) * full_gain[:, None, None]).astype(jnp.bfloat16)
    return result


def transpose_tile(pair_tile):
    depth_dim, tile_rows, tile_cols = pair_tile.shape
    across = lax.axis_size("gy")
    down_size = lax.axis_size("gx")
    quarter = tile_rows // across
    spread_rows = lax.all_to_all(pair_tile, "gy", split_axis=1, concat_axis=2, tiled=True)
    blocks = spread_rows.reshape(depth_dim, quarter, down_size, tile_rows)
    blocks = jnp.transpose(blocks, (0, 3, 2, 1))[:, :, :, None, :]
    moved_back = lax.all_to_all(
        lax.all_to_all(blocks, "gx", split_axis=2, concat_axis=2, tiled=True),
        "gy",
        split_axis=2,
        concat_axis=3,
        tiled=True,
    )
    return moved_back.reshape(depth_dim, tile_rows, tile_cols)


def fold_panels(left_tile, right_tile):
    left_panel = lax.all_gather(left_tile, "gy", axis=2, tiled=True)
    return jnp.einsum(
        "hik,hkj->hij",
        left_panel,
        lax.all_gather(right_tile, "gx", axis=1, tiled=True),
        preferred_element_type=jnp.float32,
    )


def distributed(
    pair, residue_mask, norm_in_gain, proj_weight, gate_weight, norm_out_gain, out_weight
):
    tile_rows = pair.shape[1]
    tile_cols = pair.shape[2]
    row_start = lax.axis_index("gx") * tile_rows
    col_start = lax.axis_index("gy") * tile_cols
    row_flags = lax.dynamic_slice_in_dim(residue_mask, row_start, tile_rows).astype(jnp.float32)
    col_flags = lax.dynamic_slice_in_dim(residue_mask, col_start, tile_cols).astype(jnp.float32)
    pair_mask = row_flags[:, None] * col_flags[None, :]
    current = pair
    for update in range(2):
        normed = layer_norm_gathered(current, norm_in_gain[update])
        projected = jnp.einsum(
            "cij,pch->phij", normed, proj_weight[update], preferred_element_type=jnp.float32
        )
        left_tile = (jax.nn.sigmoid(projected[0]) * projected[1] * pair_mask).astype(jnp.bfloat16)
        right_tile = (jax.nn.sigmoid(projected[2]) * projected[3] * pair_mask).astype(jnp.bfloat16)
        gate_values = jax.nn.sigmoid(
            jnp.einsum(
                "cij,cd->dij", normed, gate_weight[update], preferred_element_type=jnp.float32
            )
        )
        if update == 0:
            triangle = fold_panels(left_tile, transpose_tile(right_tile))
        else:
            triangle = fold_panels(transpose_tile(left_tile), right_tile)
        tri_normed = layer_norm_gathered(triangle, norm_out_gain[update])
        current = current + gate_values * jnp.einsum(
            "hij,hd->dij", tri_normed, out_weight[update], preferred_element_type=jnp.float32
        )
    return current


def fits_replicated(pair, residue_mask):
    part, tile_rows, tile_cols = pair.shape
    res = residue_mask.shape[0]
    return (
        lax.axis_size("gz") == 2
        and res * res * part * 2 * 4 <= REPLICATED_LIMIT
        and lax.axis_size("gy") == 2
        and lax.axis_size("gx").bit_count() == 1
        and res % 4 == 0
        and tile_rows % 2 == 0
        and tile_cols % 8 == 0
        and tile_cols % tile_rows == 0
    )


def per_device(pair, residue_mask, *parameters):
    plan = replicated if fits_replicated(pair, residue_mask) else distributed
    return plan(pair, residue_mask, *parameters)


def solution(mesh):
    return jax.shard_map(
        per_device,
        mesh=mesh,
        in_specs=(
            P(("groups", "gz"), "gx", "gy"),
            P("groups"),
            P(None, "gz"),
            P(None, None, None, "gz"),
            P(None, None, "gz"),
            P(None, "gz"),
            P(None, None, "gz"),
        ),
        out_specs=P(("groups", "gz"), "gx", "gy"),
        check_vma=False,
    )
```

```python
import functools

import jax
import jax.numpy as jnp
from jax import lax
from jax.experimental import pallas as pl
from jax.experimental.pallas import tpu as pltpu
from jax.sharding import PartitionSpec as P


EPSILON = 1e-05
F32 = jnp.float32
BF16 = jnp.bfloat16
REPLICATED_LIMIT = 4 * 1024 * 1024


def dot(x, w):
    return jnp.dot(x.astype(BF16), w, preferred_element_type=F32)


def lane_norm(x, gain, ones):
    d = x - jnp.mean(x, axis=-1, keepdims=True)
    return d * lax.rsqrt(dot(d * d, ones) + EPSILON) * gain


def gated(x, w):
    p = dot(x, w)
    ch = p.shape[1] // 2
    return (jnp.tanh(p[:, :ch]) + 1.0) * p[:, ch:]


def rows_at(first, count):
    return pl.ds(first if isinstance(first, int) else pl.multiple_of(first, 8), count)


def own_kernel(tile, out, whole):
    half = tile.shape[0] // 2
    rows = tile[pl.ds(lax.axis_index("gz") * half, half)]
    out[...] = rows.reshape(out.shape)
    whole[...] = tile[...]


def centre_kernel(own, other, out):
    core = lax.axis_index("gz")
    pairs, part = own.shape
    half = other.shape[0] // 2
    theirs = other[pl.ds(core * half, half)].reshape(pairs, part)
    both = pltpu.roll(jnp.concatenate([own[...], theirs], axis=1), core * part, 1)
    out[...] = (both - jnp.mean(both, axis=-1, keepdims=True)).astype(BF16)


def weights_kernel(own, other, own_gains, other_gains, flags, wleft, wright, wgate, wout, gains, mask):
    core = lax.axis_index("gz")
    half = own.shape[2]
    for u in range(2):
        for p in range(6):
            mine, theirs = own[u, p].astype(F32) * 0.5, other[u, p].astype(F32) * 0.5
            first = jnp.where(core == 0, mine, theirs)
            second = jnp.where(core == 0, theirs, mine)
            full = jnp.transpose(jnp.concatenate([first, second], axis=0)).astype(BF16)
            if p < 2:
                wleft[u, :, p * 2 * half : (p + 1) * 2 * half] = full
            elif p < 4:
                wright[u, :, (p - 2) * 2 * half : (p - 1) * 2 * half] = full
            elif p == 4:
                wgate[u] = full
            else:
                wout[u] = full
    gains[...] = pltpu.roll(jnp.concatenate([own_gains[...], other_gains[...]], axis=1), core * half, 1)
    row = flags[...].astype(F32)
    size = row.shape[1]
    wide = jnp.transpose(jnp.broadcast_to(row, (mask.shape[1], size)))
    mask[...] = jnp.zeros_like(mask)
    mask[:size, :] = wide


class Place:
    def __init__(self, res, tile_rows, tile_cols):
        self.res, self.rows, self.cols = res, tile_rows, tile_cols
        self.half = tile_rows // 2
        self.blocks = res // tile_rows
        self.per_column = tile_cols // tile_rows
        self.ipad = -(-tile_rows // 8) * 8
        self.span = tile_cols + self.ipad
        self.part = self.blocks * self.half
        self.row_block = lax.axis_index("gx")
        self.col_block = lax.axis_index("gy")
        self.core = lax.axis_index("gz")
        self.first_row = self.row_block * tile_rows
        self.first_col = self.col_block * tile_cols

    def which(self, own):
        return self.core if own else 1 - self.core

    def mask_rows(self, mask, own):
        return [
            mask[pl.ds((self.row_block ^ s) * self.rows + self.which(own) * self.half + q, 1), :]
            for s in range(self.blocks)
            for q in range(self.half)
        ]


def columns_part(at, source, mask, gains, wleft, wright, raw, normed, left, right, column):
    cols = at.cols
    size = at.half * cols
    ch = mask.shape[1]
    zs = []
    for s in range(at.blocks):
        x = source[s].astype(F32)
        var = jnp.mean(x * x, axis=-1, keepdims=True)
        zs.append(x * lax.rsqrt(var + EPSILON) * gains[0:1, :])
        raw[s * size : (s + 1) * size, :] = x
        normed[s * size : (s + 1) * size, :] = zs[s]
    pairs = at.part * cols
    raw[pairs:, :] = jnp.zeros((raw.shape[0] - pairs, ch), F32)
    normed[pairs:, :] = jnp.zeros((raw.shape[0] - pairs, ch), F32)
    kmask = mask[rows_at(column * cols, cols), :]
    y = gated(jnp.concatenate(zs, axis=0), wleft[0]).reshape(at.part, cols, ch) * kmask[None]
    left[...] = y.reshape(pairs, ch)
    wanted = []
    for t in range(at.per_column):
        s = at.row_block ^ (at.col_block * at.per_column + t)
        wanted.append(normed[rows_at(s * size, size), :])
    right[...] = gated(jnp.concatenate(wanted + zs[:1], axis=0), wright[0])


def place_right(at, right_own, right_other, rightt):
    cols, span = at.cols, at.span
    for k in range(at.ipad - at.rows):
        rightt[pl.ds(cols + at.rows + k, cols, stride=span), :] = jnp.zeros((cols, rightt.shape[1]), F32)
    for right, which in ((right_own, at.core), (right_other, 1 - at.core)):
        for t in range(at.per_column + 1):
            for q in range(at.half):
                first = (t * at.half + q) * cols
                slot = t * at.rows + which * at.half + q
                rightt[pl.ds(slot, cols, stride=span), :] = right[first : first + cols, :]


def triangle_phase(at, left_own, left_other, rightt, tri, start):
    cols, span = at.cols, at.span
    ch = rightt.shape[1]
    count = 4
    for left, base in ((left_own, 0), (left_other, at.part)):

        def tri_block(n, carry, left=left, base=base):
            def add(k, accs):
                r = rightt[pl.ds(pl.multiple_of(k * span, 8), span), :]
                return tuple(
                    acc + left[pl.ds((n * count + q) * cols + k, 1), :] * r for q, acc in enumerate(accs)
                )

            where = [pl.ds(pl.multiple_of((base + n * count + q) * span, 8), span) for q in range(count)]
            accs = tuple(jnp.zeros((span, ch), F32) if start is None else start[w, :] for w in where)
            accs = lax.fori_loop(0, cols, add, accs, unroll=min(cols, 24))
            for w, acc in zip(where, accs):
                tri[w, :] = acc
            return carry

        lax.fori_loop(0, at.part // count, tri_block, 0)


def near_own_kernel(source, mask, gains, wleft, wright, raw, normed, left, right, *, place):
    at = Place(*place)
    columns_part(at, source, mask, gains, wleft, wright, raw, normed, left, right, at.col_block)


def near_other_kernel(
    source, right_own, mask, gains, wleft, wright, raw, normed, left, rightt, right, *, place
):
    at = Place(*place)
    columns_part(at, source, mask, gains, wleft, wright, raw, normed, left, right, at.col_block)
    place_right(at, right_own, right, rightt)


def near_triangle_kernel(left_own, left_other, rightt, tri, *, place):
    triangle_phase(Place(*place), left_own, left_other, rightt, tri, None)


def far_own_kernel(
    source, near_own, near_other, mask, gains, wleft, wright, wgate, raw, normed, left, right, gate, *, place
):
    at = Place(*place)
    columns_part(at, source, mask, gains, wleft, wright, raw, normed, left, right, 1 - at.col_block)
    pairs = at.part * at.cols
    for n, normed_near in enumerate((near_own, near_other)):
        gate[n * pairs : (n + 1) * pairs, :] = jnp.tanh(dot(normed_near[:pairs, :], wgate[0])) + 1.0


def far_kernel(
    source, near_raws_own, near_raws_other, near_normed_own, near_normed_other, near_tri,
    raw_own, normed_own, left_own, right_own, near_gate,
    mask, gains, wleft, wright, wgate, wout, pair, out,
    raw_other, normed_other, left_other, right_other, rightt, tri, first_update, znext, right1, left1, *, place,
):
    at = Place(*place)
    res, rows, cols, ipad, span, half = at.res, at.rows, at.cols, at.ipad, at.span, at.half
    ch = mask.shape[1]
    columns_part(
        at, source, mask, gains, wleft, wright, raw_other, normed_other, left_other, right_other, 1 - at.col_block
    )
    place_right(at, right_own, right_other, rightt)
    triangle_phase(at, left_own, left_other, rightt, tri, near_tri)
    ones = jnp.full((ch, ch), 1.0 / ch, BF16)
    gain_in, gain_out = gains[0:2, :], gains[2:4, :]

    smask = jnp.concatenate(
        [mask[rows_at(at.first_col, cols), :], mask[pl.ds(at.first_row, ipad), :]], axis=0
    )
    row_is_near = at.first_row // cols == at.col_block
    offset = at.first_row % cols
    mrows = at.mask_rows(mask, True) + at.mask_rows(mask, False)
    zs, ns = [], []
    for near_raw, raw, near_normed, normed in (
        (near_raws_own, raw_own, near_normed_own, normed_own),
        (near_raws_other, raw_other, near_normed_other, normed_other),
    ):
        for r in range(at.part):
            where = pl.ds(r * cols + offset, ipad)
            zs += [near_raw[r * cols : (r + 1) * cols, :], jnp.where(row_is_near, near_raw[where, :], raw[where, :])]
            ns.append(jnp.where(row_is_near, near_normed[where, :], normed[where, :]))
    gate_rows = jnp.tanh(dot(jnp.concatenate(ns, axis=0), wgate[0])) + 1.0
    gates = []
    for r in range(res):
        m = smask * mrows[r]
        gates.append(near_gate[r * cols : (r + 1) * cols, :] * m[:cols])
        gates.append(gate_rows[r * ipad : (r + 1) * ipad] * m[cols:])
    tn = lane_norm(tri[...], gain_out[0:1], ones)
    update = jnp.concatenate(gates, axis=0) * dot(tn, wout[0])
    first_update[...] = update
    znext[...] = lane_norm(jnp.concatenate(zs, axis=0) + update, gain_in[1:2], ones)

    z3 = znext[...].reshape(res, span, ch)
    right1[...] = gated(z3[:, :cols].reshape(res * cols, ch), wright[1])
    v = gated(z3[:, cols:].reshape(res * ipad, ch), wleft[1])
    for r in range(res):
        left1[r * ipad : (r + 1) * ipad, :] = v[r * ipad : (r + 1) * ipad] * mrows[r]

    def tri1_block(k, accs):
        r = right1[pl.ds(pl.multiple_of(k * cols, 8), cols), :]
        return tuple(acc + left1[pl.ds(k * ipad + i, 1), :] * r for i, acc in enumerate(accs))

    accs = lax.fori_loop(0, res, tri1_block, tuple(jnp.zeros((cols, ch), F32) for _ in range(rows)), unroll=4)
    tn = lane_norm(jnp.concatenate(accs, axis=0), gain_out[1:2], ones)
    ns, us, ms = [], [], []
    for i in range(rows):
        local = (at.core ^ (i // half)) * at.part + i % half
        where = pl.ds(pl.multiple_of(local * span, 8), cols)
        ns.append(znext[where, :])
        us.append(first_update[where, :])
        ms.append(smask[:cols] * mask[pl.ds(at.first_row + i, 1), :])
    gate = (jnp.tanh(dot(jnp.concatenate(ns, axis=0), wgate[1])) + 1.0) * jnp.concatenate(ms, axis=0)
    part = ch // 2
    before = pltpu.roll(jnp.concatenate(us, axis=0), at.core * part, 1)
    moved = before + pltpu.roll(gate * dot(tn, wout[1]), at.core * part, 1)
    out[...] = pair[...] + moved[:, :part].reshape(rows, cols, part)


def swap(x, axis, mask=1):
    size = lax.axis_size(axis)
    return lax.ppermute(x, axis, [(i, i ^ mask) for i in range(size)])


def call(kernel, out_shape, *args, scratch=(), vmem_mib=4, flops=2**20):
    return pl.pallas_call(
        kernel,
        out_shape=out_shape,
        scratch_shapes=list(scratch),
        compiler_params=pltpu.CompilerParams(vmem_limit_bytes=vmem_mib * 1024 * 1024),
        cost_estimate=pl.CostEstimate(flops=flops, bytes_accessed=2**16, transcendentals=0),
    )(*args)


def replicated(
    pair, residue_mask, norm_in_gain, proj_weight, gate_weight, norm_out_gain, out_weight
):
    part, tile_rows, tile_cols = pair.shape
    tile = jnp.transpose(pair, (1, 2, 0))
    res = residue_mask.shape[0]
    ch = 2 * part
    half = tile_rows // 2
    ipad = -(-tile_rows // 8) * 8
    span = tile_cols + ipad
    blocks = lax.axis_size("gx")
    place = (res, tile_rows, tile_cols)
    pairs = res * tile_cols
    wide = lambda rows: jax.ShapeDtypeStruct((rows, ch), F32)
    vmem = lambda rows: pltpu.VMEM((rows, ch), F32)
    narrow = lambda *shape: jax.ShapeDtypeStruct(shape, BF16)

    other_tile = swap(tile, "gz")
    own_weights = jnp.concatenate(
        [
            jnp.transpose(proj_weight, (0, 1, 3, 2)),
            jnp.transpose(gate_weight, (0, 2, 1))[:, None],
            jnp.transpose(out_weight, (0, 2, 1))[:, None],
        ],
        axis=1,
    )
    own_gains = jnp.concatenate([norm_in_gain, norm_out_gain], axis=0)
    other_weights = swap(own_weights, "gz")
    other_gains = swap(own_gains, "gz")

    own_rows, kept_tile = call(
        own_kernel, [jax.ShapeDtypeStruct((half * tile_cols, part), F32), jax.ShapeDtypeStruct(tile.shape, F32)], tile
    )
    message = call(centre_kernel, narrow(half * tile_cols, ch), own_rows, other_tile)
    column = [message]
    for s in range(1, blocks):
        column.append(swap(message, "gx", s))
    wleft, wright, wgate, wout, gains, mask = call(
        weights_kernel,
        [narrow(2, ch, 2 * ch), narrow(2, ch, 2 * ch), narrow(2, ch, ch), narrow(2, ch, ch), wide(4), wide(res + 8)],
        own_weights, other_weights, own_gains, other_gains, residue_mask[None, :],
        vmem_mib=8,
    )
    near = jnp.stack(column)
    far = swap(near, "gy")
    near_other = swap(near, "gz")
    far_other = swap(far, "gz")
    part_pairs = pairs // 2
    right_rows = (tile_cols + tile_rows) // 2 * tile_cols
    part_shapes = [wide(part_pairs + 8), wide(part_pairs + 8), wide(part_pairs), wide(right_rows)]
    parameters = (mask, gains, wleft, wright)
    raw_own, normed_own, left_own, right_own = call(
        functools.partial(near_own_kernel, place=place),
        part_shapes,
        near, *parameters,
        flops=2**24,
    )
    raw_other, normed_other, left_other, near_right = call(
        functools.partial(near_other_kernel, place=place),
        part_shapes[:3] + [wide(tile_cols * span)],
        near_other, right_own, *parameters,
        scratch=[vmem(right_rows)],
        flops=2**24,
    )
    near_tri = call(
        functools.partial(near_triangle_kernel, place=place),
        wide(res * span),
        left_own, left_other, near_right,
        flops=2**26,
    )
    *far_parts, near_gate = call(
        functools.partial(far_own_kernel, place=place),
        part_shapes + [wide(pairs)],
        far, normed_own, normed_other, *parameters, wgate,
        flops=2**24,
    )
    result = call(
        functools.partial(far_kernel, place=place),
        jax.ShapeDtypeStruct(tile.shape, F32),
        far_other, raw_own, raw_other, normed_own, normed_other, near_tri, *far_parts, near_gate,
        *parameters, wgate, wout, kept_tile,
        scratch=[
            vmem(part_pairs + 8),
            vmem(part_pairs + 8),
            vmem(part_pairs),
            vmem(right_rows),
            vmem(tile_cols * span),
            vmem(res * span),
            vmem(res * span),
            vmem(res * span),
            vmem(pairs),
            vmem(res * ipad),
        ],
        vmem_mib=20,
    )
    return jnp.transpose(result, (2, 0, 1))


def layer_norm_gathered(values, gain_part):
    full_values, full_gain = (
        lax.all_gather(values, "gz", axis=0, tiled=True),
        lax.all_gather(gain_part, "gz", axis=0, tiled=True),
    )
    mean_val = jnp.mean(full_values, axis=0)
    centred = full_values - mean_val
    spread = jnp.mean(centred * centred, axis=0)
    result = (centred * lax.rsqrt(spread + EPSILON) * full_gain[:, None, None]).astype(jnp.bfloat16)
    return result


def transpose_tile(pair_tile):
    depth_dim, tile_rows, tile_cols = pair_tile.shape
    across = lax.axis_size("gy")
    down_size = lax.axis_size("gx")
    quarter = tile_rows // across
    spread_rows = lax.all_to_all(pair_tile, "gy", split_axis=1, concat_axis=2, tiled=True)
    blocks = spread_rows.reshape(depth_dim, quarter, down_size, tile_rows)
    blocks = jnp.transpose(blocks, (0, 3, 2, 1))[:, :, :, None, :]
    moved_back = lax.all_to_all(
        lax.all_to_all(blocks, "gx", split_axis=2, concat_axis=2, tiled=True),
        "gy",
        split_axis=2,
        concat_axis=3,
        tiled=True,
    )
    return moved_back.reshape(depth_dim, tile_rows, tile_cols)


def fold_panels(left_tile, right_tile):
    left_panel = lax.all_gather(left_tile, "gy", axis=2, tiled=True)
    return jnp.einsum(
        "hik,hkj->hij",
        left_panel,
        lax.all_gather(right_tile, "gx", axis=1, tiled=True),
        preferred_element_type=jnp.float32,
    )


def distributed(
    pair, residue_mask, norm_in_gain, proj_weight, gate_weight, norm_out_gain, out_weight
):
    tile_rows = pair.shape[1]
    tile_cols = pair.shape[2]
    row_start = lax.axis_index("gx") * tile_rows
    col_start = lax.axis_index("gy") * tile_cols
    row_flags = lax.dynamic_slice_in_dim(residue_mask, row_start, tile_rows).astype(jnp.float32)
    col_flags = lax.dynamic_slice_in_dim(residue_mask, col_start, tile_cols).astype(jnp.float32)
    pair_mask = row_flags[:, None] * col_flags[None, :]
    current = pair
    for update in range(2):
        normed = layer_norm_gathered(current, norm_in_gain[update])
        projected = jnp.einsum(
            "cij,pch->phij", normed, proj_weight[update], preferred_element_type=jnp.float32
        )
        left_tile = (jax.nn.sigmoid(projected[0]) * projected[1] * pair_mask).astype(jnp.bfloat16)
        right_tile = (jax.nn.sigmoid(projected[2]) * projected[3] * pair_mask).astype(jnp.bfloat16)
        gate_values = jax.nn.sigmoid(
            jnp.einsum(
                "cij,cd->dij", normed, gate_weight[update], preferred_element_type=jnp.float32
            )
        )
        if update == 0:
            triangle = fold_panels(left_tile, transpose_tile(right_tile))
        else:
            triangle = fold_panels(transpose_tile(left_tile), right_tile)
        tri_normed = layer_norm_gathered(triangle, norm_out_gain[update])
        current = current + gate_values * jnp.einsum(
            "hij,hd->dij", tri_normed, out_weight[update], preferred_element_type=jnp.float32
        )
    return current


def fits_replicated(pair, residue_mask):
    part, tile_rows, tile_cols = pair.shape
    res = residue_mask.shape[0]
    return (
        lax.axis_size("gz") == 2
        and res * res * part * 2 * 4 <= REPLICATED_LIMIT
        and lax.axis_size("gy") == 2
        and lax.axis_size("gx").bit_count() == 1
        and res % 8 == 0
        and res // tile_rows * (tile_rows // 2) % 4 == 0
        and tile_rows % 2 == 0
        and tile_cols % 8 == 0
        and tile_cols % tile_rows == 0
    )


def per_device(pair, residue_mask, *parameters):
    plan = replicated if fits_replicated(pair, residue_mask) else distributed
    return plan(pair, residue_mask, *parameters)


def solution(mesh):
    return jax.shard_map(
        per_device,
        mesh=mesh,
        in_specs=(
            P(("groups", "gz"), "gx", "gy"),
            P("groups"),
            P(None, "gz"),
            P(None, None, None, "gz"),
            P(None, None, "gz"),
            P(None, "gz"),
            P(None, None, "gz"),
        ),
        out_specs=P(("groups", "gz"), "gx", "gy"),
        check_vma=False,
    )
```

```python
import functools

import jax
import jax.numpy as jnp
from jax import lax
from jax.experimental import pallas as pl
from jax.experimental.pallas import tpu as pltpu
from jax.sharding import PartitionSpec as P


EPSILON = 1e-05
F32 = jnp.float32
BF16 = jnp.bfloat16
REPLICATED_LIMIT = 4 * 1024 * 1024


def dot(x, w):
    return jnp.dot(x.astype(BF16), w, preferred_element_type=F32)


def lane_norm(x, gain, ones=None):
    d = x - jnp.mean(x, axis=-1, keepdims=True)
    var = jnp.mean(d * d, axis=-1, keepdims=True) if ones is None else dot(d * d, ones)
    return d * lax.rsqrt(var + EPSILON) * gain


def gated(x, w):
    p = dot(x, w)
    ch = p.shape[1] // 2
    return (jnp.tanh(p[:, :ch]) + 1.0) * p[:, ch:]


def rows_at(first, count):
    return pl.ds(first if isinstance(first, int) else pl.multiple_of(first, 8), count)


def own_kernel(tile, out, whole):
    half = tile.shape[0] // 2
    rows = tile[pl.ds(lax.axis_index("gz") * half, half)]
    out[...] = rows.reshape(out.shape)
    whole[...] = tile[...]


def centre_kernel(own, other, out):
    core = lax.axis_index("gz")
    pairs, part = own.shape
    half = other.shape[0] // 2
    theirs = other[pl.ds(core * half, half)].reshape(pairs, part)
    both = pltpu.roll(jnp.concatenate([own[...], theirs], axis=1), core * part, 1)
    out[...] = (both - jnp.mean(both, axis=-1, keepdims=True)).astype(BF16)


def weights_kernel(own, other, own_gains, other_gains, flags, wleft, wright, wgate, wout, gains, mask):
    core = lax.axis_index("gz")
    half = own.shape[2]
    for u in range(2):
        for p in range(6):
            mine, theirs = own[u, p].astype(F32) * 0.5, other[u, p].astype(F32) * 0.5
            natural = (core == 0) | (u == 1 and p >= 4)
            first = jnp.where(natural, mine, theirs)
            second = jnp.where(natural, theirs, mine)
            full = jnp.transpose(jnp.concatenate([first, second], axis=0)).astype(BF16)
            if p < 2:
                wleft[u, :, p * 2 * half : (p + 1) * 2 * half] = full
            elif p < 4:
                wright[u, :, (p - 2) * 2 * half : (p - 1) * 2 * half] = full
            elif p == 4:
                wgate[u] = full
            else:
                wout[u] = full
    gains[...] = pltpu.roll(jnp.concatenate([own_gains[...], other_gains[...]], axis=1), core * half, 1)
    row = flags[...].astype(F32)
    size = row.shape[1]
    wide = jnp.transpose(jnp.broadcast_to(row, (mask.shape[1], size)))
    mask[...] = jnp.zeros_like(mask)
    mask[:size, :] = wide


class Place:
    def __init__(self, res, tile_rows, tile_cols):
        self.res, self.rows, self.cols = res, tile_rows, tile_cols
        self.half = tile_rows // 2
        self.blocks = res // tile_rows
        self.per_column = tile_cols // tile_rows
        self.ipad = -(-tile_rows // 8) * 8
        self.span = tile_cols + self.ipad
        self.part = self.blocks * self.half
        self.row_block = lax.axis_index("gx")
        self.col_block = lax.axis_index("gy")
        self.core = lax.axis_index("gz")
        self.first_row = self.row_block * tile_rows
        self.first_col = self.col_block * tile_cols

    def which(self, own):
        return self.core if own else 1 - self.core

    def mask_rows(self, mask, own):
        return [
            mask[pl.ds((self.row_block ^ s) * self.rows + self.which(own) * self.half + q, 1), :]
            for s in range(self.blocks)
            for q in range(self.half)
        ]


def columns_part(at, source, mask, gains, wleft, wright, raw, normed, left, right, column):
    cols = at.cols
    size = at.half * cols
    ch = mask.shape[1]
    zs = []
    for s in range(at.blocks):
        x = source[s].astype(F32)
        var = jnp.mean(x * x, axis=-1, keepdims=True)
        zs.append(x * lax.rsqrt(var + EPSILON) * gains[0:1, :])
        raw[s * size : (s + 1) * size, :] = x
        normed[s * size : (s + 1) * size, :] = zs[s]
    pairs = at.part * cols
    raw[pairs:, :] = jnp.zeros((raw.shape[0] - pairs, ch), F32)
    normed[pairs:, :] = jnp.zeros((raw.shape[0] - pairs, ch), F32)
    kmask = mask[rows_at(column * cols, cols), :]
    y = gated(jnp.concatenate(zs, axis=0), wleft[0]).reshape(at.part, cols, ch) * kmask[None]
    left[...] = y.reshape(pairs, ch)
    wanted = []
    for t in range(at.per_column):
        s = at.row_block ^ (at.col_block * at.per_column + t)
        wanted.append(normed[rows_at(s * size, size), :])
    right[...] = gated(jnp.concatenate(wanted + zs[:1], axis=0), wright[0])


def place_right(at, right_own, right_other, rightt):
    cols, span = at.cols, at.span
    for k in range(at.ipad - at.rows):
        rightt[pl.ds(cols + at.rows + k, cols, stride=span), :] = jnp.zeros((cols, rightt.shape[1]), F32)
    for right, which in ((right_own, at.core), (right_other, 1 - at.core)):
        for t in range(at.per_column + 1):
            for q in range(at.half):
                first = (t * at.half + q) * cols
                slot = t * at.rows + which * at.half + q
                rightt[pl.ds(slot, cols, stride=span), :] = right[first : first + cols, :]


def triangle_phase(at, left_own, left_other, rightt, tri, start):
    cols, span = at.cols, at.span
    ch = rightt.shape[1]
    count = 4
    for left, base in ((left_own, 0), (left_other, at.part)):

        def tri_block(n, carry, left=left, base=base):
            def add(k, accs):
                r = rightt[pl.ds(pl.multiple_of(k * span, 8), span), :]
                return tuple(
                    acc + left[pl.ds((n * count + q) * cols + k, 1), :] * r for q, acc in enumerate(accs)
                )

            where = [pl.ds(pl.multiple_of((base + n * count + q) * span, 8), span) for q in range(count)]
            accs = tuple(jnp.zeros((span, ch), F32) if start is None else start[w, :] for w in where)
            accs = lax.fori_loop(0, cols, add, accs, unroll=min(cols, 24))
            for w, acc in zip(where, accs):
                tri[w, :] = acc
            return carry

        lax.fori_loop(0, at.part // count, tri_block, 0)


def near_own_kernel(source, mask, gains, wleft, wright, raw, normed, left, right, *, place):
    at = Place(*place)
    columns_part(at, source, mask, gains, wleft, wright, raw, normed, left, right, at.col_block)


def near_other_kernel(
    source, right_own, mask, gains, wleft, wright, raw, normed, left, rightt, right, *, place
):
    at = Place(*place)
    columns_part(at, source, mask, gains, wleft, wright, raw, normed, left, right, at.col_block)
    place_right(at, right_own, right, rightt)


def near_triangle_kernel(left_own, left_other, rightt, tri, *, place):
    triangle_phase(Place(*place), left_own, left_other, rightt, tri, None)


def far_own_kernel(
    source, near_own, near_other, mask, gains, wleft, wright, wgate, raw, normed, left, right, gate, *, place
):
    at = Place(*place)
    columns_part(at, source, mask, gains, wleft, wright, raw, normed, left, right, 1 - at.col_block)
    pairs = at.part * at.cols
    for n, normed_near in enumerate((near_own, near_other)):
        gate[n * pairs : (n + 1) * pairs, :] = jnp.tanh(dot(normed_near[:pairs, :], wgate[0])) + 1.0


def far_kernel(
    source, near_raws_own, near_raws_other, near_normed_own, near_normed_other, near_tri,
    raw_own, normed_own, left_own, right_own, near_gate,
    mask, gains, wleft, wright, wgate, wout, pair, out,
    raw_other, normed_other, left_other, right_other, rightt, tri, first_update, znext, right1, left1, *, place,
):
    at = Place(*place)
    res, rows, cols, ipad, span, half = at.res, at.rows, at.cols, at.ipad, at.span, at.half
    ch = mask.shape[1]
    columns_part(
        at, source, mask, gains, wleft, wright, raw_other, normed_other, left_other, right_other, 1 - at.col_block
    )
    place_right(at, right_own, right_other, rightt)
    triangle_phase(at, left_own, left_other, rightt, tri, near_tri)
    ones = jnp.full((ch, ch), 1.0 / ch, BF16)
    gain_in, gain_out = gains[0:2, :], gains[2:4, :]

    smask = jnp.concatenate(
        [mask[rows_at(at.first_col, cols), :], mask[pl.ds(at.first_row, ipad), :]], axis=0
    )
    row_is_near = at.first_row // cols == at.col_block
    offset = at.first_row % cols
    mrows = at.mask_rows(mask, True) + at.mask_rows(mask, False)
    zs, ns = [], []
    for near_raw, raw, near_normed, normed in (
        (near_raws_own, raw_own, near_normed_own, normed_own),
        (near_raws_other, raw_other, near_normed_other, normed_other),
    ):
        for r in range(at.part):
            where = pl.ds(r * cols + offset, ipad)
            zs += [near_raw[r * cols : (r + 1) * cols, :], jnp.where(row_is_near, near_raw[where, :], raw[where, :])]
            ns.append(jnp.where(row_is_near, near_normed[where, :], normed[where, :]))
    gate_rows = jnp.tanh(dot(jnp.concatenate(ns, axis=0), wgate[0])) + 1.0
    gates = []
    for r in range(res):
        m = smask * mrows[r]
        gates.append(near_gate[r * cols : (r + 1) * cols, :] * m[:cols])
        gates.append(gate_rows[r * ipad : (r + 1) * ipad] * m[cols:])
    tn = lane_norm(tri[...], gain_out[0:1], ones)
    update = jnp.concatenate(gates, axis=0) * dot(tn, wout[0])
    first_update[...] = update
    znext[...] = lane_norm(jnp.concatenate(zs, axis=0) + update, gain_in[1:2], ones)

    z3 = znext[...].reshape(res, span, ch)
    right1[...] = gated(z3[:, :cols].reshape(res * cols, ch), wright[1])
    v = gated(z3[:, cols:].reshape(res * ipad, ch), wleft[1])
    for r in range(res):
        left1[r * ipad : (r + 1) * ipad, :] = v[r * ipad : (r + 1) * ipad] * mrows[r]

    def tri1_block(k, accs):
        r = right1[pl.ds(pl.multiple_of(k * cols, 8), cols), :]
        return tuple(acc + left1[pl.ds(k * ipad + i, 1), :] * r for i, acc in enumerate(accs))

    accs = lax.fori_loop(0, res, tri1_block, tuple(jnp.zeros((cols, ch), F32) for _ in range(rows)), unroll=12 if res % 12 == 0 else 4)
    tn = lane_norm(jnp.concatenate(accs, axis=0), gain_out[1:2])
    ns, us, ms = [], [], []
    for i in range(rows):
        local = (at.core ^ (i // half)) * at.part + i % half
        where = pl.ds(pl.multiple_of(local * span, 8), cols)
        ns.append(znext[where, :])
        us.append(first_update[where, :])
        ms.append(smask[:cols] * mask[pl.ds(at.first_row + i, 1), :])
    gate = (jnp.tanh(dot(jnp.concatenate(ns, axis=0), wgate[1])) + 1.0) * jnp.concatenate(ms, axis=0)
    part = ch // 2
    before = pltpu.roll(jnp.concatenate(us, axis=0), at.core * part, 1)
    moved = before + gate * dot(tn, wout[1])
    out[...] = pair[...] + moved[:, :part].reshape(rows, cols, part)


def swap(x, axis, mask=1):
    size = lax.axis_size(axis)
    return lax.ppermute(x, axis, [(i, i ^ mask) for i in range(size)])


def call(kernel, out_shape, *args, scratch=(), vmem_mib=4, flops=2**20):
    return pl.pallas_call(
        kernel,
        out_shape=out_shape,
        scratch_shapes=list(scratch),
        compiler_params=pltpu.CompilerParams(vmem_limit_bytes=vmem_mib * 1024 * 1024),
        cost_estimate=pl.CostEstimate(flops=flops, bytes_accessed=2**16, transcendentals=0),
    )(*args)


def replicated(
    pair, residue_mask, norm_in_gain, proj_weight, gate_weight, norm_out_gain, out_weight
):
    part, tile_rows, tile_cols = pair.shape
    tile = jnp.transpose(pair, (1, 2, 0))
    res = residue_mask.shape[0]
    ch = 2 * part
    half = tile_rows // 2
    ipad = -(-tile_rows // 8) * 8
    span = tile_cols + ipad
    blocks = lax.axis_size("gx")
    place = (res, tile_rows, tile_cols)
    pairs = res * tile_cols
    wide = lambda rows: jax.ShapeDtypeStruct((rows, ch), F32)
    vmem = lambda rows: pltpu.VMEM((rows, ch), F32)
    narrow = lambda *shape: jax.ShapeDtypeStruct(shape, BF16)

    other_tile = swap(tile, "gz")
    own_weights = jnp.concatenate(
        [
            jnp.transpose(proj_weight, (0, 1, 3, 2)),
            jnp.transpose(gate_weight, (0, 2, 1))[:, None],
            jnp.transpose(out_weight, (0, 2, 1))[:, None],
        ],
        axis=1,
    )
    own_gains = jnp.concatenate([norm_in_gain, norm_out_gain], axis=0)
    other_weights = swap(own_weights, "gz")
    other_gains = swap(own_gains, "gz")

    own_rows, kept_tile = call(
        own_kernel, [jax.ShapeDtypeStruct((half * tile_cols, part), F32), jax.ShapeDtypeStruct(tile.shape, F32)], tile
    )
    message = call(centre_kernel, narrow(half * tile_cols, ch), own_rows, other_tile)
    column = [message]
    for s in range(1, blocks):
        column.append(swap(message, "gx", s))
    wleft, wright, wgate, wout, gains, mask = call(
        weights_kernel,
        [narrow(2, ch, 2 * ch), narrow(2, ch, 2 * ch), narrow(2, ch, ch), narrow(2, ch, ch), wide(4), wide(res + 8)],
        own_weights, other_weights, own_gains, other_gains, residue_mask[None, :],
        vmem_mib=8,
    )
    near = jnp.stack(column)
    far = swap(near, "gy")
    near_other = swap(near, "gz")
    far_other = swap(far, "gz")
    part_pairs = pairs // 2
    right_rows = (tile_cols + tile_rows) // 2 * tile_cols
    part_shapes = [wide(part_pairs + 8), wide(part_pairs + 8), wide(part_pairs), wide(right_rows)]
    parameters = (mask, gains, wleft, wright)
    raw_own, normed_own, left_own, right_own = call(
        functools.partial(near_own_kernel, place=place),
        part_shapes,
        near, *parameters,
        flops=2**24,
    )
    raw_other, normed_other, left_other, near_right = call(
        functools.partial(near_other_kernel, place=place),
        part_shapes[:3] + [wide(tile_cols * span)],
        near_other, right_own, *parameters,
        scratch=[vmem(right_rows)],
        flops=2**24,
    )
    near_tri = call(
        functools.partial(near_triangle_kernel, place=place),
        wide(res * span),
        left_own, left_other, near_right,
        flops=2**26,
    )
    *far_parts, near_gate = call(
        functools.partial(far_own_kernel, place=place),
        part_shapes + [wide(pairs)],
        far, normed_own, normed_other, *parameters, wgate,
        flops=2**24,
    )
    result = call(
        functools.partial(far_kernel, place=place),
        jax.ShapeDtypeStruct(tile.shape, F32),
        far_other, raw_own, raw_other, normed_own, normed_other, near_tri, *far_parts, near_gate,
        *parameters, wgate, wout, kept_tile,
        scratch=[
            vmem(part_pairs + 8),
            vmem(part_pairs + 8),
            vmem(part_pairs),
            vmem(right_rows),
            vmem(tile_cols * span),
            vmem(res * span),
            vmem(res * span),
            vmem(res * span),
            vmem(pairs),
            vmem(res * ipad),
        ],
        vmem_mib=20,
    )
    return jnp.transpose(result, (2, 0, 1))


def layer_norm_gathered(values, gain_part):
    full_values, full_gain = (
        lax.all_gather(values, "gz", axis=0, tiled=True),
        lax.all_gather(gain_part, "gz", axis=0, tiled=True),
    )
    mean_val = jnp.mean(full_values, axis=0)
    centred = full_values - mean_val
    spread = jnp.mean(centred * centred, axis=0)
    result = (centred * lax.rsqrt(spread + EPSILON) * full_gain[:, None, None]).astype(jnp.bfloat16)
    return result


def transpose_tile(pair_tile):
    depth_dim, tile_rows, tile_cols = pair_tile.shape
    across = lax.axis_size("gy")
    down_size = lax.axis_size("gx")
    quarter = tile_rows // across
    spread_rows = lax.all_to_all(pair_tile, "gy", split_axis=1, concat_axis=2, tiled=True)
    blocks = spread_rows.reshape(depth_dim, quarter, down_size, tile_rows)
    blocks = jnp.transpose(blocks, (0, 3, 2, 1))[:, :, :, None, :]
    moved_back = lax.all_to_all(
        lax.all_to_all(blocks, "gx", split_axis=2, concat_axis=2, tiled=True),
        "gy",
        split_axis=2,
        concat_axis=3,
        tiled=True,
    )
    return moved_back.reshape(depth_dim, tile_rows, tile_cols)


def fold_panels(left_tile, right_tile):
    left_panel = lax.all_gather(left_tile, "gy", axis=2, tiled=True)
    return jnp.einsum(
        "hik,hkj->hij",
        left_panel,
        lax.all_gather(right_tile, "gx", axis=1, tiled=True),
        preferred_element_type=jnp.float32,
    )


def distributed(
    pair, residue_mask, norm_in_gain, proj_weight, gate_weight, norm_out_gain, out_weight
):
    tile_rows = pair.shape[1]
    tile_cols = pair.shape[2]
    row_start = lax.axis_index("gx") * tile_rows
    col_start = lax.axis_index("gy") * tile_cols
    row_flags = lax.dynamic_slice_in_dim(residue_mask, row_start, tile_rows).astype(jnp.float32)
    col_flags = lax.dynamic_slice_in_dim(residue_mask, col_start, tile_cols).astype(jnp.float32)
    pair_mask = row_flags[:, None] * col_flags[None, :]
    current = pair
    for update in range(2):
        normed = layer_norm_gathered(current, norm_in_gain[update])
        projected = jnp.einsum(
            "cij,pch->phij", normed, proj_weight[update], preferred_element_type=jnp.float32
        )
        left_tile = (jax.nn.sigmoid(projected[0]) * projected[1] * pair_mask).astype(jnp.bfloat16)
        right_tile = (jax.nn.sigmoid(projected[2]) * projected[3] * pair_mask).astype(jnp.bfloat16)
        gate_values = jax.nn.sigmoid(
            jnp.einsum(
                "cij,cd->dij", normed, gate_weight[update], preferred_element_type=jnp.float32
            )
        )
        if update == 0:
            triangle = fold_panels(left_tile, transpose_tile(right_tile))
        else:
            triangle = fold_panels(transpose_tile(left_tile), right_tile)
        tri_normed = layer_norm_gathered(triangle, norm_out_gain[update])
        current = current + gate_values * jnp.einsum(
            "hij,hd->dij", tri_normed, out_weight[update], preferred_element_type=jnp.float32
        )
    return current


def fits_replicated(pair, residue_mask):
    part, tile_rows, tile_cols = pair.shape
    res = residue_mask.shape[0]
    return (
        lax.axis_size("gz") == 2
        and res * res * part * 2 * 4 <= REPLICATED_LIMIT
        and lax.axis_size("gy") == 2
        and lax.axis_size("gx").bit_count() == 1
        and res % 8 == 0
        and res // tile_rows * (tile_rows // 2) % 4 == 0
        and tile_rows % 2 == 0
        and tile_cols % 8 == 0
        and tile_cols % tile_rows == 0
    )


def per_device(pair, residue_mask, *parameters):
    plan = replicated if fits_replicated(pair, residue_mask) else distributed
    return plan(pair, residue_mask, *parameters)


def solution(mesh):
    return jax.shard_map(
        per_device,
        mesh=mesh,
        in_specs=(
            P(("groups", "gz"), "gx", "gy"),
            P("groups"),
            P(None, "gz"),
            P(None, None, None, "gz"),
            P(None, None, "gz"),
            P(None, "gz"),
            P(None, None, "gz"),
        ),
        out_specs=P(("groups", "gz"), "gx", "gy"),
        check_vma=False,
    )
```

```python
import functools

import jax
import jax.numpy as jnp
from jax import lax
from jax.experimental import pallas as pl
from jax.experimental.pallas import tpu as pltpu
from jax.sharding import PartitionSpec as P


EPSILON = 1e-05
F32 = jnp.float32
BF16 = jnp.bfloat16
REPLICATED_LIMIT = 4 * 1024 * 1024


def dot(x, w):
    return jnp.dot(x.astype(BF16), w, preferred_element_type=F32)


def lane_norm(x, gain, ones=None):
    d = x - jnp.mean(x, axis=-1, keepdims=True)
    var = jnp.mean(d * d, axis=-1, keepdims=True) if ones is None else dot(d * d, ones)
    return d * lax.rsqrt(var + EPSILON) * gain


def gated(x, w):
    p = dot(x, w)
    ch = p.shape[1] // 2
    return (jnp.tanh(p[:, :ch]) + 1.0) * p[:, ch:]


def rows_at(first, count):
    return pl.ds(first if isinstance(first, int) else pl.multiple_of(first, 8), count)


def own_kernel(tile, out, whole):
    half = tile.shape[0] // 2
    rows = tile[pl.ds(lax.axis_index("gz") * half, half)]
    out[...] = rows.reshape(out.shape)
    whole[...] = tile[...]


def centre_kernel(own, other, out):
    core = lax.axis_index("gz")
    pairs, part = own.shape
    half = other.shape[0] // 2
    theirs = other[pl.ds(core * half, half)].reshape(pairs, part)
    both = pltpu.roll(jnp.concatenate([own[...], theirs], axis=1), core * part, 1)
    out[...] = (both - jnp.mean(both, axis=-1, keepdims=True)).astype(BF16)


def weights_kernel(own, other, own_gains, other_gains, flags, wleft, wright, wgate, wout, gains, mask):
    core = lax.axis_index("gz")
    half = own.shape[2]
    for u in range(2):
        for p in range(6):
            mine, theirs = own[u, p].astype(F32) * 0.5, other[u, p].astype(F32) * 0.5
            natural = (core == 0) | (u == 1 and p >= 4)
            first = jnp.where(natural, mine, theirs)
            second = jnp.where(natural, theirs, mine)
            full = jnp.transpose(jnp.concatenate([first, second], axis=0)).astype(BF16)
            if p < 2:
                wleft[u, :, p * 2 * half : (p + 1) * 2 * half] = full
            elif p < 4:
                wright[u, :, (p - 2) * 2 * half : (p - 1) * 2 * half] = full
            elif p == 4:
                wgate[u] = full
            else:
                wout[u] = full
    gains[...] = pltpu.roll(jnp.concatenate([own_gains[...], other_gains[...]], axis=1), core * half, 1)
    row = flags[...].astype(F32)
    size = row.shape[1]
    wide = jnp.transpose(jnp.broadcast_to(row, (mask.shape[1], size)))
    mask[...] = jnp.zeros_like(mask)
    mask[:size, :] = wide


class Place:
    def __init__(self, res, tile_rows, tile_cols):
        self.res, self.rows, self.cols = res, tile_rows, tile_cols
        self.half = tile_rows // 2
        self.blocks = res // tile_rows
        self.per_column = tile_cols // tile_rows
        self.ipad = -(-tile_rows // 8) * 8
        self.span = tile_cols + self.ipad
        self.part = self.blocks * self.half
        self.row_block = lax.axis_index("gx")
        self.col_block = lax.axis_index("gy")
        self.core = lax.axis_index("gz")
        self.first_row = self.row_block * tile_rows
        self.first_col = self.col_block * tile_cols

    def which(self, own):
        return self.core if own else 1 - self.core

    def mask_rows(self, mask, own):
        return [
            mask[pl.ds((self.row_block ^ s) * self.rows + self.which(own) * self.half + q, 1), :]
            for s in range(self.blocks)
            for q in range(self.half)
        ]


def columns_part(at, source, mask, gains, wleft, wright, raw, normed, left, right, column):
    cols = at.cols
    size = at.half * cols
    ch = mask.shape[1]
    zs = []
    for s in range(at.blocks):
        x = source[s].astype(F32)
        var = jnp.mean(x * x, axis=-1, keepdims=True)
        zs.append(x * lax.rsqrt(var + EPSILON) * gains[0:1, :])
        raw[s * size : (s + 1) * size, :] = x
        normed[s * size : (s + 1) * size, :] = zs[s]
    pairs = at.part * cols
    raw[pairs:, :] = jnp.zeros((raw.shape[0] - pairs, ch), F32)
    normed[pairs:, :] = jnp.zeros((raw.shape[0] - pairs, ch), F32)
    kmask = mask[rows_at(column * cols, cols), :]
    y = gated(jnp.concatenate(zs, axis=0), wleft[0]).reshape(at.part, cols, ch) * kmask[None]
    left[...] = y.reshape(pairs, ch)
    wanted = []
    for t in range(at.per_column):
        s = at.row_block ^ (at.col_block * at.per_column + t)
        wanted.append(normed[rows_at(s * size, size), :])
    right[...] = gated(jnp.concatenate(wanted + zs[:1], axis=0), wright[0])


def place_right(at, right_own, right_other, rightt):
    cols, span = at.cols, at.span
    for k in range(at.ipad - at.rows):
        rightt[pl.ds(cols + at.rows + k, cols, stride=span), :] = jnp.zeros((cols, rightt.shape[1]), F32)
    for right, which in ((right_own, at.core), (right_other, 1 - at.core)):
        for t in range(at.per_column + 1):
            for q in range(at.half):
                first = (t * at.half + q) * cols
                slot = t * at.rows + which * at.half + q
                rightt[pl.ds(slot, cols, stride=span), :] = right[first : first + cols, :]


def triangle_phase(at, left, rightt, tri, base, start):
    cols, span = at.cols, at.span
    ch = rightt.shape[1]
    count = 4

    def tri_block(n, carry):
        def add(k, accs):
            r = rightt[pl.ds(pl.multiple_of(k * span, 8), span), :]
            return tuple(acc + left[pl.ds((n * count + q) * cols + k, 1), :] * r for q, acc in enumerate(accs))

        where = [pl.multiple_of((n * count + q) * span, 8) for q in range(count)]
        accs = tuple(jnp.zeros((span, ch), F32) if start is None else start[pl.ds(w, span), :] for w in where)
        accs = lax.fori_loop(0, cols, add, accs, unroll=min(cols, 24))
        for w, acc in zip(where, accs):
            tri[pl.ds(base * span + w, span), :] = acc
        return carry

    lax.fori_loop(0, at.part // count, tri_block, 0, unroll=3 if at.part // count % 3 == 0 else 1)


def near_own_kernel(source, mask, gains, wleft, wright, raw, normed, left, right, *, place):
    at = Place(*place)
    columns_part(at, source, mask, gains, wleft, wright, raw, normed, left, right, at.col_block)


def near_other_kernel(
    source, right_own, mask, gains, wleft, wright, raw, normed, left, rightt, right, *, place
):
    at = Place(*place)
    columns_part(at, source, mask, gains, wleft, wright, raw, normed, left, right, at.col_block)
    place_right(at, right_own, right, rightt)


def near_triangle_kernel(left, rightt, tri, *, place):
    triangle_phase(Place(*place), left, rightt, tri, 0, None)


def far_own_kernel(
    source, near_own, near_other, mask, gains, wleft, wright, wgate, raw, normed, left, right, gate, *, place
):
    at = Place(*place)
    columns_part(at, source, mask, gains, wleft, wright, raw, normed, left, right, 1 - at.col_block)
    pairs = at.part * at.cols
    for n, normed_near in enumerate((near_own, near_other)):
        gate[n * pairs : (n + 1) * pairs, :] = jnp.tanh(dot(normed_near[:pairs, :], wgate[0])) + 1.0


def far_kernel(
    source, near_raws_own, near_raws_other, near_normed_own, near_normed_other, near_tri_own, near_tri_other,
    raw_own, normed_own, left_own, right_own, near_gate,
    mask, gains, wleft, wright, wgate, wout, pair, out,
    raw_other, normed_other, left_other, right_other, rightt, tri, first_update, znext, right1, left1, *, place,
):
    at = Place(*place)
    res, rows, cols, ipad, span, half = at.res, at.rows, at.cols, at.ipad, at.span, at.half
    ch = mask.shape[1]
    columns_part(
        at, source, mask, gains, wleft, wright, raw_other, normed_other, left_other, right_other, 1 - at.col_block
    )
    place_right(at, right_own, right_other, rightt)
    triangle_phase(at, left_own, rightt, tri, 0, near_tri_own)
    triangle_phase(at, left_other, rightt, tri, at.part, near_tri_other)
    ones = jnp.full((ch, ch), 1.0 / ch, BF16)
    gain_in, gain_out = gains[0:2, :], gains[2:4, :]

    smask = jnp.concatenate(
        [mask[rows_at(at.first_col, cols), :], mask[pl.ds(at.first_row, ipad), :]], axis=0
    )
    row_is_near = at.first_row // cols == at.col_block
    offset = at.first_row % cols
    mrows = at.mask_rows(mask, True) + at.mask_rows(mask, False)
    zs, ns = [], []
    for near_raw, raw, near_normed, normed in (
        (near_raws_own, raw_own, near_normed_own, normed_own),
        (near_raws_other, raw_other, near_normed_other, normed_other),
    ):
        for r in range(at.part):
            where = pl.ds(r * cols + offset, ipad)
            zs += [near_raw[r * cols : (r + 1) * cols, :], jnp.where(row_is_near, near_raw[where, :], raw[where, :])]
            ns.append(jnp.where(row_is_near, near_normed[where, :], normed[where, :]))
    gate_rows = jnp.tanh(dot(jnp.concatenate(ns, axis=0), wgate[0])) + 1.0
    gates = []
    for r in range(res):
        m = smask * mrows[r]
        gates.append(near_gate[r * cols : (r + 1) * cols, :] * m[:cols])
        gates.append(gate_rows[r * ipad : (r + 1) * ipad] * m[cols:])
    tn = lane_norm(tri[...], gain_out[0:1], ones)
    update = jnp.concatenate(gates, axis=0) * dot(tn, wout[0])
    first_update[...] = update
    znext[...] = lane_norm(jnp.concatenate(zs, axis=0) + update, gain_in[1:2], ones)

    z3 = znext[...].reshape(res, span, ch)
    right1[...] = gated(z3[:, :cols].reshape(res * cols, ch), wright[1])
    v = gated(z3[:, cols:].reshape(res * ipad, ch), wleft[1])
    for r in range(res):
        left1[r * ipad : (r + 1) * ipad, :] = v[r * ipad : (r + 1) * ipad] * mrows[r]

    def tri1_block(k, accs):
        r = right1[pl.ds(pl.multiple_of(k * cols, 8), cols), :]
        return tuple(acc + left1[pl.ds(k * ipad + i, 1), :] * r for i, acc in enumerate(accs))

    accs = lax.fori_loop(0, res, tri1_block, tuple(jnp.zeros((cols, ch), F32) for _ in range(rows)), unroll=12 if res % 12 == 0 else 4)
    tn = lane_norm(jnp.concatenate(accs, axis=0), gain_out[1:2])
    ns, us, ms = [], [], []
    for i in range(rows):
        local = (at.core ^ (i // half)) * at.part + i % half
        where = pl.ds(pl.multiple_of(local * span, 8), cols)
        ns.append(znext[where, :])
        us.append(first_update[where, :])
        ms.append(smask[:cols] * mask[pl.ds(at.first_row + i, 1), :])
    gate = (jnp.tanh(dot(jnp.concatenate(ns, axis=0), wgate[1])) + 1.0) * jnp.concatenate(ms, axis=0)
    part = ch // 2
    before = pltpu.roll(jnp.concatenate(us, axis=0), at.core * part, 1)
    moved = before + gate * dot(tn, wout[1])
    out[...] = pair[...] + moved[:, :part].reshape(rows, cols, part)


def swap(x, axis, mask=1):
    size = lax.axis_size(axis)
    return lax.ppermute(x, axis, [(i, i ^ mask) for i in range(size)])


def call(kernel, out_shape, *args, scratch=(), vmem_mib=4, flops=2**20):
    return pl.pallas_call(
        kernel,
        out_shape=out_shape,
        scratch_shapes=list(scratch),
        compiler_params=pltpu.CompilerParams(vmem_limit_bytes=vmem_mib * 1024 * 1024),
        cost_estimate=pl.CostEstimate(flops=flops, bytes_accessed=2**16, transcendentals=0),
    )(*args)


def replicated(
    pair, residue_mask, norm_in_gain, proj_weight, gate_weight, norm_out_gain, out_weight
):
    part, tile_rows, tile_cols = pair.shape
    tile = jnp.transpose(pair, (1, 2, 0))
    res = residue_mask.shape[0]
    ch = 2 * part
    half = tile_rows // 2
    ipad = -(-tile_rows // 8) * 8
    span = tile_cols + ipad
    blocks = lax.axis_size("gx")
    place = (res, tile_rows, tile_cols)
    pairs = res * tile_cols
    wide = lambda rows: jax.ShapeDtypeStruct((rows, ch), F32)
    vmem = lambda rows: pltpu.VMEM((rows, ch), F32)
    narrow = lambda *shape: jax.ShapeDtypeStruct(shape, BF16)

    other_tile = swap(tile, "gz")
    own_weights = jnp.concatenate(
        [
            jnp.transpose(proj_weight, (0, 1, 3, 2)),
            jnp.transpose(gate_weight, (0, 2, 1))[:, None],
            jnp.transpose(out_weight, (0, 2, 1))[:, None],
        ],
        axis=1,
    )
    own_gains = jnp.concatenate([norm_in_gain, norm_out_gain], axis=0)
    other_weights = swap(own_weights, "gz")
    other_gains = swap(own_gains, "gz")

    own_rows, kept_tile = call(
        own_kernel, [jax.ShapeDtypeStruct((half * tile_cols, part), F32), jax.ShapeDtypeStruct(tile.shape, F32)], tile
    )
    message = call(centre_kernel, narrow(half * tile_cols, ch), own_rows, other_tile)
    column = [message]
    for s in range(1, blocks):
        column.append(swap(message, "gx", s))
    wleft, wright, wgate, wout, gains, mask = call(
        weights_kernel,
        [narrow(2, ch, 2 * ch), narrow(2, ch, 2 * ch), narrow(2, ch, ch), narrow(2, ch, ch), wide(4), wide(res + 8)],
        own_weights, other_weights, own_gains, other_gains, residue_mask[None, :],
        vmem_mib=8,
    )
    near = jnp.stack(column)
    far_first = swap(message, "gy")
    far_rest = swap(jnp.stack(column[1:]), "gy")
    far = jnp.concatenate([far_first[None], far_rest], axis=0)
    near_other = swap(near, "gz")
    far_other = swap(far, "gz")
    part_pairs = pairs // 2
    right_rows = (tile_cols + tile_rows) // 2 * tile_cols
    part_shapes = [wide(part_pairs + 8), wide(part_pairs + 8), wide(part_pairs), wide(right_rows)]
    parameters = (mask, gains, wleft, wright)
    raw_own, normed_own, left_own, right_own = call(
        functools.partial(near_own_kernel, place=place),
        part_shapes,
        near, *parameters,
        flops=2**24,
    )
    raw_other, normed_other, left_other, near_right = call(
        functools.partial(near_other_kernel, place=place),
        part_shapes[:3] + [wide(tile_cols * span)],
        near_other, right_own, *parameters,
        scratch=[vmem(right_rows)],
        flops=2**24,
    )
    near_tris = []
    for left in (left_own, left_other):
        near_tris.append(
            call(
                functools.partial(near_triangle_kernel, place=place),
                wide(res // 2 * span),
                left, near_right,
                flops=2**25,
            )
        )
    *far_parts, near_gate = call(
        functools.partial(far_own_kernel, place=place),
        part_shapes + [wide(pairs)],
        far, normed_own, normed_other, *parameters, wgate,
        flops=2**24,
    )
    result = call(
        functools.partial(far_kernel, place=place),
        jax.ShapeDtypeStruct(tile.shape, F32),
        far_other, raw_own, raw_other, normed_own, normed_other, *near_tris, *far_parts, near_gate,
        *parameters, wgate, wout, kept_tile,
        scratch=[
            vmem(part_pairs + 8),
            vmem(part_pairs + 8),
            vmem(part_pairs),
            vmem(right_rows),
            vmem(tile_cols * span),
            vmem(res * span),
            vmem(res * span),
            vmem(res * span),
            vmem(pairs),
            vmem(res * ipad),
        ],
        vmem_mib=20,
    )
    return jnp.transpose(result, (2, 0, 1))


def layer_norm_gathered(values, gain_part):
    full_values, full_gain = (
        lax.all_gather(values, "gz", axis=0, tiled=True),
        lax.all_gather(gain_part, "gz", axis=0, tiled=True),
    )
    mean_val = jnp.mean(full_values, axis=0)
    centred = full_values - mean_val
    spread = jnp.mean(centred * centred, axis=0)
    result = (centred * lax.rsqrt(spread + EPSILON) * full_gain[:, None, None]).astype(jnp.bfloat16)
    return result


def transpose_tile(pair_tile):
    depth_dim, tile_rows, tile_cols = pair_tile.shape
    across = lax.axis_size("gy")
    down_size = lax.axis_size("gx")
    quarter = tile_rows // across
    spread_rows = lax.all_to_all(pair_tile, "gy", split_axis=1, concat_axis=2, tiled=True)
    blocks = spread_rows.reshape(depth_dim, quarter, down_size, tile_rows)
    blocks = jnp.transpose(blocks, (0, 3, 2, 1))[:, :, :, None, :]
    moved_back = lax.all_to_all(
        lax.all_to_all(blocks, "gx", split_axis=2, concat_axis=2, tiled=True),
        "gy",
        split_axis=2,
        concat_axis=3,
        tiled=True,
    )
    return moved_back.reshape(depth_dim, tile_rows, tile_cols)


def fold_panels(left_tile, right_tile):
    left_panel = lax.all_gather(left_tile, "gy", axis=2, tiled=True)
    return jnp.einsum(
        "hik,hkj->hij",
        left_panel,
        lax.all_gather(right_tile, "gx", axis=1, tiled=True),
        preferred_element_type=jnp.float32,
    )


def distributed(
    pair, residue_mask, norm_in_gain, proj_weight, gate_weight, norm_out_gain, out_weight
):
    tile_rows = pair.shape[1]
    tile_cols = pair.shape[2]
    row_start = lax.axis_index("gx") * tile_rows
    col_start = lax.axis_index("gy") * tile_cols
    row_flags = lax.dynamic_slice_in_dim(residue_mask, row_start, tile_rows).astype(jnp.float32)
    col_flags = lax.dynamic_slice_in_dim(residue_mask, col_start, tile_cols).astype(jnp.float32)
    pair_mask = row_flags[:, None] * col_flags[None, :]
    current = pair
    for update in range(2):
        normed = layer_norm_gathered(current, norm_in_gain[update])
        projected = jnp.einsum(
            "cij,pch->phij", normed, proj_weight[update], preferred_element_type=jnp.float32
        )
        left_tile = (jax.nn.sigmoid(projected[0]) * projected[1] * pair_mask).astype(jnp.bfloat16)
        right_tile = (jax.nn.sigmoid(projected[2]) * projected[3] * pair_mask).astype(jnp.bfloat16)
        gate_values = jax.nn.sigmoid(
            jnp.einsum(
                "cij,cd->dij", normed, gate_weight[update], preferred_element_type=jnp.float32
            )
        )
        if update == 0:
            triangle = fold_panels(left_tile, transpose_tile(right_tile))
        else:
            triangle = fold_panels(transpose_tile(left_tile), right_tile)
        tri_normed = layer_norm_gathered(triangle, norm_out_gain[update])
        current = current + gate_values * jnp.einsum(
            "hij,hd->dij", tri_normed, out_weight[update], preferred_element_type=jnp.float32
        )
    return current


def fits_replicated(pair, residue_mask):
    part, tile_rows, tile_cols = pair.shape
    res = residue_mask.shape[0]
    return (
        lax.axis_size("gz") == 2
        and res * res * part * 2 * 4 <= REPLICATED_LIMIT
        and lax.axis_size("gy") == 2
        and lax.axis_size("gx").bit_count() == 1
        and res % 8 == 0
        and res // tile_rows * (tile_rows // 2) % 4 == 0
        and tile_rows % 2 == 0
        and tile_cols % 8 == 0
        and tile_cols % tile_rows == 0
    )


def per_device(pair, residue_mask, *parameters):
    plan = replicated if fits_replicated(pair, residue_mask) else distributed
    return plan(pair, residue_mask, *parameters)


def solution(mesh):
    return jax.shard_map(
        per_device,
        mesh=mesh,
        in_specs=(
            P(("groups", "gz"), "gx", "gy"),
            P("groups"),
            P(None, "gz"),
            P(None, None, None, "gz"),
            P(None, None, "gz"),
            P(None, "gz"),
            P(None, None, "gz"),
        ),
        out_specs=P(("groups", "gz"), "gx", "gy"),
        check_vma=False,
    )
```

```python
import functools

import jax
import jax.numpy as jnp
from jax import lax
from jax.experimental import pallas as pl
from jax.experimental.pallas import tpu as pltpu
from jax.sharding import PartitionSpec as P


EPSILON = 1e-05
F32 = jnp.float32
BF16 = jnp.bfloat16
REPLICATED_LIMIT = 4 * 1024 * 1024


def dot(x, w):
    return jnp.dot(x.astype(BF16), w, preferred_element_type=F32)


def lane_norm(x, gain, ones=None):
    d = x - jnp.mean(x, axis=-1, keepdims=True)
    var = jnp.mean(d * d, axis=-1, keepdims=True) if ones is None else dot(d * d, ones)
    return d * lax.rsqrt(var + EPSILON) * gain


def gated(x, w):
    p = dot(x, w)
    ch = p.shape[1] // 2
    return (jnp.tanh(p[:, :ch]) + 1.0) * p[:, ch:]


def rows_at(first, count):
    return pl.ds(first if isinstance(first, int) else pl.multiple_of(first, 8), count)


def own_kernel(tile, out, whole):
    half = tile.shape[0] // 2
    rows = tile[pl.ds(lax.axis_index("gz") * half, half)]
    out[...] = rows.reshape(out.shape)
    whole[...] = tile[...]


def centre_kernel(own, other, out):
    core = lax.axis_index("gz")
    pairs, part = own.shape
    half = other.shape[0] // 2
    theirs = other[pl.ds(core * half, half)].reshape(pairs, part)
    both = pltpu.roll(jnp.concatenate([own[...], theirs], axis=1), core * part, 1)
    out[...] = (both - jnp.mean(both, axis=-1, keepdims=True)).astype(BF16)


def weights_kernel(own, other, own_gains, other_gains, flags, wleft, wright, wgate, wout, gains, mask):
    core = lax.axis_index("gz")
    half = own.shape[2]
    for u in range(2):
        for p in range(6):
            mine, theirs = own[u, p].astype(F32) * 0.5, other[u, p].astype(F32) * 0.5
            natural = (core == 0) | (u == 1 and p >= 4)
            first = jnp.where(natural, mine, theirs)
            second = jnp.where(natural, theirs, mine)
            full = jnp.transpose(jnp.concatenate([first, second], axis=0)).astype(BF16)
            if p < 2:
                wleft[u, :, p * 2 * half : (p + 1) * 2 * half] = full
            elif p < 4:
                wright[u, :, (p - 2) * 2 * half : (p - 1) * 2 * half] = full
            elif p == 4:
                wgate[u] = full
            else:
                wout[u] = full
    gains[...] = pltpu.roll(jnp.concatenate([own_gains[...], other_gains[...]], axis=1), core * half, 1)
    row = flags[...].astype(F32)
    size = row.shape[1]
    wide = jnp.transpose(jnp.broadcast_to(row, (mask.shape[1], size)))
    mask[...] = jnp.zeros_like(mask)
    mask[:size, :] = wide


class Place:
    def __init__(self, res, tile_rows, tile_cols):
        self.res, self.rows, self.cols = res, tile_rows, tile_cols
        self.half = tile_rows // 2
        self.blocks = res // tile_rows
        self.per_column = tile_cols // tile_rows
        self.ipad = -(-tile_rows // 8) * 8
        self.span = tile_cols + self.ipad
        self.part = self.blocks * self.half
        self.row_block = lax.axis_index("gx")
        self.col_block = lax.axis_index("gy")
        self.core = lax.axis_index("gz")
        self.first_row = self.row_block * tile_rows
        self.first_col = self.col_block * tile_cols

    def which(self, own):
        return self.core if own else 1 - self.core

    def mask_rows(self, mask, own):
        return [
            mask[pl.ds((self.row_block ^ s) * self.rows + self.which(own) * self.half + q, 1), :]
            for s in range(self.blocks)
            for q in range(self.half)
        ]


def columns_part(at, source, mask, gains, wleft, wright, raw, normed, left, right, column):
    cols = at.cols
    size = at.half * cols
    ch = mask.shape[1]
    zs = []
    for s in range(at.blocks):
        x = source[s].astype(F32)
        var = jnp.mean(x * x, axis=-1, keepdims=True)
        zs.append(x * lax.rsqrt(var + EPSILON) * gains[0:1, :])
        raw[s * size : (s + 1) * size, :] = x
        normed[s * size : (s + 1) * size, :] = zs[s]
    pairs = at.part * cols
    raw[pairs:, :] = jnp.zeros((raw.shape[0] - pairs, ch), F32)
    normed[pairs:, :] = jnp.zeros((raw.shape[0] - pairs, ch), F32)
    kmask = mask[rows_at(column * cols, cols), :]
    y = gated(jnp.concatenate(zs, axis=0), wleft[0]).reshape(at.part, cols, ch) * kmask[None]
    left[...] = y.reshape(pairs, ch)
    wanted = []
    for t in range(at.per_column):
        s = at.row_block ^ (at.col_block * at.per_column + t)
        wanted.append(normed[rows_at(s * size, size), :])
    right[...] = gated(jnp.concatenate(wanted + zs[:1], axis=0), wright[0])


def place_right(at, right_own, right_other, rightt):
    cols, span = at.cols, at.span
    for k in range(at.ipad - at.rows):
        rightt[pl.ds(cols + at.rows + k, cols, stride=span), :] = jnp.zeros((cols, rightt.shape[1]), F32)
    for right, which in ((right_own, at.core), (right_other, 1 - at.core)):
        for t in range(at.per_column + 1):
            for q in range(at.half):
                first = (t * at.half + q) * cols
                slot = t * at.rows + which * at.half + q
                rightt[pl.ds(slot, cols, stride=span), :] = right[first : first + cols, :]


def triangle_phase(at, left, rightt, tri, base, start):
    cols, span = at.cols, at.span
    ch = rightt.shape[1]
    count = 4

    def tri_block(n, carry):
        def add(k, accs):
            r = rightt[pl.ds(pl.multiple_of(k * span, 8), span), :]
            return tuple(acc + left[pl.ds((n * count + q) * cols + k, 1), :] * r for q, acc in enumerate(accs))

        where = [pl.multiple_of((n * count + q) * span, 8) for q in range(count)]
        accs = tuple(jnp.zeros((span, ch), F32) if start is None else start[pl.ds(w, span), :] for w in where)
        accs = lax.fori_loop(0, cols, add, accs, unroll=min(cols, 24))
        for w, acc in zip(where, accs):
            tri[pl.ds(base * span + w, span), :] = acc
        return carry

    lax.fori_loop(0, at.part // count, tri_block, 0, unroll=3 if at.part // count % 3 == 0 else 1)


def near_own_kernel(source, mask, gains, wleft, wright, raw, normed, left, right, *, place):
    at = Place(*place)
    columns_part(at, source, mask, gains, wleft, wright, raw, normed, left, right, at.col_block)


def near_other_kernel(
    source, right_own, mask, gains, wleft, wright, raw, normed, left, rightt, right, *, place
):
    at = Place(*place)
    columns_part(at, source, mask, gains, wleft, wright, raw, normed, left, right, at.col_block)
    place_right(at, right_own, right, rightt)


def near_triangle_kernel(left, rightt, tri, *, place):
    triangle_phase(Place(*place), left, rightt, tri, 0, None)


def far_own_kernel(
    source, near_own, near_other, mask, gains, wleft, wright, wgate, raw, normed, left, right, gate, *, place
):
    at = Place(*place)
    columns_part(at, source, mask, gains, wleft, wright, raw, normed, left, right, 1 - at.col_block)
    pairs = at.part * at.cols
    for n, normed_near in enumerate((near_own, near_other)):
        gate[n * pairs : (n + 1) * pairs, :] = jnp.tanh(dot(normed_near[:pairs, :], wgate[0])) + 1.0


def far_kernel(
    source, near_raws_own, near_raws_other, near_normed_own, near_normed_other, near_tri_own, near_tri_other,
    raw_own, normed_own, left_own, right_own, near_gate,
    mask, gains, wleft, wright, wgate, wout, pair, out,
    raw_other, normed_other, left_other, right_other, rightt, tri, first_update, znext, right1, left1, *, place,
):
    at = Place(*place)
    res, rows, cols, ipad, span, half = at.res, at.rows, at.cols, at.ipad, at.span, at.half
    ch = mask.shape[1]
    columns_part(
        at, source, mask, gains, wleft, wright, raw_other, normed_other, left_other, right_other, 1 - at.col_block
    )
    place_right(at, right_own, right_other, rightt)
    triangle_phase(at, left_own, rightt, tri, 0, near_tri_own)
    triangle_phase(at, left_other, rightt, tri, at.part, near_tri_other)
    ones = jnp.full((ch, ch), 1.0 / ch, BF16)
    gain_in, gain_out = gains[0:2, :], gains[2:4, :]

    smask = jnp.concatenate(
        [mask[rows_at(at.first_col, cols), :], mask[pl.ds(at.first_row, ipad), :]], axis=0
    )
    row_is_near = at.first_row // cols == at.col_block
    offset = at.first_row % cols
    mrows = at.mask_rows(mask, True) + at.mask_rows(mask, False)
    zs, ns = [], []
    for near_raw, raw, near_normed, normed in (
        (near_raws_own, raw_own, near_normed_own, normed_own),
        (near_raws_other, raw_other, near_normed_other, normed_other),
    ):
        for r in range(at.part):
            where = pl.ds(r * cols + offset, ipad)
            zs += [near_raw[r * cols : (r + 1) * cols, :], jnp.where(row_is_near, near_raw[where, :], raw[where, :])]
            ns.append(jnp.where(row_is_near, near_normed[where, :], normed[where, :]))
    gate_rows = jnp.tanh(dot(jnp.concatenate(ns, axis=0), wgate[0])) + 1.0
    gates = []
    for r in range(res):
        m = smask * mrows[r]
        gates.append(near_gate[r * cols : (r + 1) * cols, :] * m[:cols])
        gates.append(gate_rows[r * ipad : (r + 1) * ipad] * m[cols:])
    tn = lane_norm(tri[...], gain_out[0:1], ones)
    update = jnp.concatenate(gates, axis=0) * dot(tn, wout[0])
    first_update[...] = update
    znext[...] = lane_norm(jnp.concatenate(zs, axis=0) + update, gain_in[1:2], ones)

    z3 = znext[...].reshape(res, span, ch)
    right1[...] = gated(z3[:, :cols].reshape(res * cols, ch), wright[1])
    v = gated(z3[:, cols:].reshape(res * ipad, ch), wleft[1])
    for r in range(res):
        left1[r * ipad : (r + 1) * ipad, :] = v[r * ipad : (r + 1) * ipad] * mrows[r]

    def tri1_block(k, accs):
        r = right1[pl.ds(pl.multiple_of(k * cols, 8), cols), :]
        return tuple(acc + left1[pl.ds(k * ipad + i, 1), :] * r for i, acc in enumerate(accs))

    accs = lax.fori_loop(0, res, tri1_block, tuple(jnp.zeros((cols, ch), F32) for _ in range(rows)), unroll=12 if res % 12 == 0 else 4)
    tn = lane_norm(jnp.concatenate(accs, axis=0), gain_out[1:2])
    ns, us, ms = [], [], []
    for i in range(rows):
        local = (at.core ^ (i // half)) * at.part + i % half
        where = pl.ds(pl.multiple_of(local * span, 8), cols)
        ns.append(znext[where, :])
        us.append(first_update[where, :])
        ms.append(smask[:cols] * mask[pl.ds(at.first_row + i, 1), :])
    gate = (jnp.tanh(dot(jnp.concatenate(ns, axis=0), wgate[1])) + 1.0) * jnp.concatenate(ms, axis=0)
    part = ch // 2
    before = pltpu.roll(jnp.concatenate(us, axis=0), at.core * part, 1)
    moved = before + gate * dot(tn, wout[1])
    out[...] = pair[...] + moved[:, :part].reshape(rows, cols, part)


def swap(x, axis, mask=1):
    size = lax.axis_size(axis)
    return lax.ppermute(x, axis, [(i, i ^ mask) for i in range(size)])


def call(kernel, out_shape, *args, scratch=(), vmem_mib=4, flops=2**20):
    return pl.pallas_call(
        kernel,
        out_shape=out_shape,
        scratch_shapes=list(scratch),
        compiler_params=pltpu.CompilerParams(vmem_limit_bytes=vmem_mib * 1024 * 1024),
        cost_estimate=pl.CostEstimate(flops=flops, bytes_accessed=2**16, transcendentals=0),
    )(*args)


def replicated(
    pair, residue_mask, norm_in_gain, proj_weight, gate_weight, norm_out_gain, out_weight
):
    part, tile_rows, tile_cols = pair.shape
    tile = jnp.transpose(pair, (1, 2, 0))
    res = residue_mask.shape[0]
    ch = 2 * part
    half = tile_rows // 2
    ipad = -(-tile_rows // 8) * 8
    span = tile_cols + ipad
    blocks = lax.axis_size("gx")
    place = (res, tile_rows, tile_cols)
    pairs = res * tile_cols
    wide = lambda rows: jax.ShapeDtypeStruct((rows, ch), F32)
    vmem = lambda rows: pltpu.VMEM((rows, ch), F32)
    narrow = lambda *shape: jax.ShapeDtypeStruct(shape, BF16)

    other_tile = swap(tile, "gz")
    own_weights = jnp.concatenate(
        [
            jnp.transpose(proj_weight, (0, 1, 3, 2)),
            jnp.transpose(gate_weight, (0, 2, 1))[:, None],
            jnp.transpose(out_weight, (0, 2, 1))[:, None],
        ],
        axis=1,
    )
    own_gains = jnp.concatenate([norm_in_gain, norm_out_gain], axis=0)
    other_weights = swap(own_weights, "gz")
    other_gains = swap(own_gains, "gz")

    own_rows, kept_tile = call(
        own_kernel, [jax.ShapeDtypeStruct((half * tile_cols, part), F32), jax.ShapeDtypeStruct(tile.shape, F32)], tile
    )
    message = call(centre_kernel, narrow(half * tile_cols, ch), own_rows, other_tile)
    column = [message]
    for s in range(1, blocks):
        column.append(swap(message, "gx", s))
    wleft, wright, wgate, wout, gains, mask = call(
        weights_kernel,
        [narrow(2, ch, 2 * ch), narrow(2, ch, 2 * ch), narrow(2, ch, ch), narrow(2, ch, ch), wide(4), wide(res + 8)],
        own_weights, other_weights, own_gains, other_gains, residue_mask[None, :],
        vmem_mib=8,
    )
    near = jnp.stack(column)
    far_first = swap(message, "gy")
    early = 2 % blocks
    far_second = swap(column[early], "gy")
    rest = [s for s in range(1, blocks) if s != early]
    far_rest = swap(jnp.stack([column[s] for s in rest]), "gy")
    arrived = {0: far_first, early: far_second}
    arrived.update({s: far_rest[n] for n, s in enumerate(rest)})
    far = jnp.stack([arrived[s] for s in range(blocks)])
    near_other = swap(near, "gz")
    far_other = swap(far, "gz")
    part_pairs = pairs // 2
    right_rows = (tile_cols + tile_rows) // 2 * tile_cols
    part_shapes = [wide(part_pairs + 8), wide(part_pairs + 8), wide(part_pairs), wide(right_rows)]
    parameters = (mask, gains, wleft, wright)
    raw_own, normed_own, left_own, right_own = call(
        functools.partial(near_own_kernel, place=place),
        part_shapes,
        near, *parameters,
        flops=2**24,
    )
    raw_other, normed_other, left_other, near_right = call(
        functools.partial(near_other_kernel, place=place),
        part_shapes[:3] + [wide(tile_cols * span)],
        near_other, right_own, *parameters,
        scratch=[vmem(right_rows)],
        flops=2**24,
    )
    near_tris = []
    for left in (left_own, left_other):
        near_tris.append(
            call(
                functools.partial(near_triangle_kernel, place=place),
                wide(res // 2 * span),
                left, near_right,
                flops=2**25,
            )
        )
    *far_parts, near_gate = call(
        functools.partial(far_own_kernel, place=place),
        part_shapes + [wide(pairs)],
        far, normed_own, normed_other, *parameters, wgate,
        flops=2**24,
    )
    result = call(
        functools.partial(far_kernel, place=place),
        jax.ShapeDtypeStruct(tile.shape, F32),
        far_other, raw_own, raw_other, normed_own, normed_other, *near_tris, *far_parts, near_gate,
        *parameters, wgate, wout, kept_tile,
        scratch=[
            vmem(part_pairs + 8),
            vmem(part_pairs + 8),
            vmem(part_pairs),
            vmem(right_rows),
            vmem(tile_cols * span),
            vmem(res * span),
            vmem(res * span),
            vmem(res * span),
            vmem(pairs),
            vmem(res * ipad),
        ],
        vmem_mib=20,
    )
    return jnp.transpose(result, (2, 0, 1))


def layer_norm_gathered(values, gain_part):
    full_values, full_gain = (
        lax.all_gather(values, "gz", axis=0, tiled=True),
        lax.all_gather(gain_part, "gz", axis=0, tiled=True),
    )
    mean_val = jnp.mean(full_values, axis=0)
    centred = full_values - mean_val
    spread = jnp.mean(centred * centred, axis=0)
    result = (centred * lax.rsqrt(spread + EPSILON) * full_gain[:, None, None]).astype(jnp.bfloat16)
    return result


def transpose_tile(pair_tile):
    depth_dim, tile_rows, tile_cols = pair_tile.shape
    across = lax.axis_size("gy")
    down_size = lax.axis_size("gx")
    quarter = tile_rows // across
    spread_rows = lax.all_to_all(pair_tile, "gy", split_axis=1, concat_axis=2, tiled=True)
    blocks = spread_rows.reshape(depth_dim, quarter, down_size, tile_rows)
    blocks = jnp.transpose(blocks, (0, 3, 2, 1))[:, :, :, None, :]
    moved_back = lax.all_to_all(
        lax.all_to_all(blocks, "gx", split_axis=2, concat_axis=2, tiled=True),
        "gy",
        split_axis=2,
        concat_axis=3,
        tiled=True,
    )
    return moved_back.reshape(depth_dim, tile_rows, tile_cols)


def fold_panels(left_tile, right_tile):
    left_panel = lax.all_gather(left_tile, "gy", axis=2, tiled=True)
    return jnp.einsum(
        "hik,hkj->hij",
        left_panel,
        lax.all_gather(right_tile, "gx", axis=1, tiled=True),
        preferred_element_type=jnp.float32,
    )


def distributed(
    pair, residue_mask, norm_in_gain, proj_weight, gate_weight, norm_out_gain, out_weight
):
    tile_rows = pair.shape[1]
    tile_cols = pair.shape[2]
    row_start = lax.axis_index("gx") * tile_rows
    col_start = lax.axis_index("gy") * tile_cols
    row_flags = lax.dynamic_slice_in_dim(residue_mask, row_start, tile_rows).astype(jnp.float32)
    col_flags = lax.dynamic_slice_in_dim(residue_mask, col_start, tile_cols).astype(jnp.float32)
    pair_mask = row_flags[:, None] * col_flags[None, :]
    current = pair
    for update in range(2):
        normed = layer_norm_gathered(current, norm_in_gain[update])
        projected = jnp.einsum(
            "cij,pch->phij", normed, proj_weight[update], preferred_element_type=jnp.float32
        )
        left_tile = (jax.nn.sigmoid(projected[0]) * projected[1] * pair_mask).astype(jnp.bfloat16)
        right_tile = (jax.nn.sigmoid(projected[2]) * projected[3] * pair_mask).astype(jnp.bfloat16)
        gate_values = jax.nn.sigmoid(
            jnp.einsum(
                "cij,cd->dij", normed, gate_weight[update], preferred_element_type=jnp.float32
            )
        )
        if update == 0:
            triangle = fold_panels(left_tile, transpose_tile(right_tile))
        else:
            triangle = fold_panels(transpose_tile(left_tile), right_tile)
        tri_normed = layer_norm_gathered(triangle, norm_out_gain[update])
        current = current + gate_values * jnp.einsum(
            "hij,hd->dij", tri_normed, out_weight[update], preferred_element_type=jnp.float32
        )
    return current


def fits_replicated(pair, residue_mask):
    part, tile_rows, tile_cols = pair.shape
    res = residue_mask.shape[0]
    return (
        lax.axis_size("gz") == 2
        and res * res * part * 2 * 4 <= REPLICATED_LIMIT
        and lax.axis_size("gy") == 2
        and lax.axis_size("gx").bit_count() == 1
        and lax.axis_size("gx") >= 4
        and res % 8 == 0
        and res // tile_rows * (tile_rows // 2) % 4 == 0
        and tile_rows % 2 == 0
        and tile_cols % 8 == 0
        and tile_cols % tile_rows == 0
    )


def per_device(pair, residue_mask, *parameters):
    plan = replicated if fits_replicated(pair, residue_mask) else distributed
    return plan(pair, residue_mask, *parameters)


def solution(mesh):
    return jax.shard_map(
        per_device,
        mesh=mesh,
        in_specs=(
            P(("groups", "gz"), "gx", "gy"),
            P("groups"),
            P(None, "gz"),
            P(None, None, None, "gz"),
            P(None, None, "gz"),
            P(None, "gz"),
            P(None, None, "gz"),
        ),
        out_specs=P(("groups", "gz"), "gx", "gy"),
        check_vma=False,
    )
```
